256 devices in a mesh: ka: 8 (over z_hi, x), band: 32 (over y, z_lo, core).
Axes of the slice: x: 4, y: 4, z: 8 (z_hi: 2, z_lo: 4; z = z_hi * 4 + z_lo), core: 2. Of those that a mesh axis runs over, the one named last changes fastest.
Arguments:
- psi_hat: float32 [8, 12, 2, 128, 128, 128], P('ka', None, None, 'band'), may hold values from -1.5 to 1.5
- occupations: int32 [8, 12], P('ka'), may hold values from 0 to 2
- weights: int32 [8], P('ka'), may hold values from 1 to 6
- density_in: float32 [128, 128, 128], P('band'), may hold values from -12 to 12
- dens_hist: float32 [8, 128, 128, 128], P(None, 'band'), may hold values from -3 to 3
- resid_hist: float32 [8, 128, 128, 128], P(None, 'band'), may hold values from -12 to 12
Outputs:
- out_density: float32 [128, 128, 128], P('band')
- mixed_density: float32 [128, 128, 128], P('band')
The draws below stay inside these ranges and needn't reach their ends.
All inputs are finite; a program needn't handle non-finite values.
Results may differ from the reference program's by a relative error of at most 0.0003.
Values sent between devices are 32-bit elements; how exact they have to be, the bound alone decides.
A program may use at most 128 MiB of HBM per device.

```python
from functools import partial
import jax
import jax.numpy as jnp
from jax import lax

NG = 128
BANDS = 12
HIST = 8
KPTS = 8


def common_field(key):
    return jax.random.truncated_normal(jax.random.fold_in(key, 7), -5.0, 5.0, (NG, NG, NG), jnp.float32)


def draw_density_in(key, part):
    shared = common_field(key)
    noise_part = jax.random.truncated_normal(jax.random.fold_in(key, 11), -5.0, 5.0, (NG, NG, NG), jnp.float32)
    return shared + 0.3 * noise_part


def draw_resid_hist(key, part):
    shared = common_field(key)
    loadings = jax.random.uniform(jax.random.fold_in(key, 13), (HIST, 1, 1, 1), jnp.float32, -1.0, 1.0)
    noise_part = jax.random.truncated_normal(jax.random.fold_in(key, 17), -5.0, 5.0, (HIST, NG, NG, NG), jnp.float32)
    return loadings * shared + 0.5 * noise_part


def touch_ends(array, stream_key, least, largest):
    longest = array.shape.index(max(array.shape))
    spots = []
    for shift in (0, 1):
        where = [jax.random.randint(jax.random.fold_in(stream_key, axis), (), 0, length) for axis, length in enumerate(array.shape)]
        where[longest] = (where[longest] + shift) % array.shape[longest]
        spots.append(tuple(where))
    return array.at[spots[0]].set(least).at[spots[1]].set(largest)


def level_of(stream_key, dims, split, smallest, top_value):
    level = 1.0
    for dim, parts in split:
        heights = jax.random.uniform(jax.random.fold_in(jax.random.fold_in(stream_key, 6), dim), (parts,), jnp.float32, smallest / len(split), top_value / len(split))
        level = level * jnp.repeat(jnp.exp(heights), dims[dim] // parts).reshape((-1,) + (1,) * (len(dims) - 1 - dim))
    return level


def gaussian(stream_key, shape, deviation, most, cuts=(), kind=jnp.bfloat16):
    gain = level_of(stream_key, shape, cuts, -0.22, 0.18) if cuts else 1.0
    result = jax.random.normal(stream_key, shape, jnp.float32) * deviation * gain
    return jnp.minimum(jnp.maximum(result, -most), most).astype(kind)


def setup_inputs(seed: int = 0) -> dict:
    key_list = jax.random.split(jax.random.key(seed), 7)
    psi_hat = gaussian(key_list[0], (KPTS, BANDS, 2, NG, NG, NG), 0.25, 1.5, ((0, 8), (3, 32)), jnp.float32)
    occupations = touch_ends(jax.random.randint(key_list[1], (KPTS, BANDS), 0, 3), jax.random.fold_in(key_list[1], 1), 0, 2).astype(jnp.int32)
    weights = touch_ends(jax.random.randint(key_list[2], (KPTS,), 1, 7), jax.random.fold_in(key_list[2], 1), 1, 6).astype(jnp.int32)
    density_in = draw_density_in(jax.random.fold_in(key_list[6], 71), 0)
    dens_hist = gaussian(key_list[4], (HIST, NG, NG, NG), 0.5, 3.0, ((1, 32),), jnp.float32)
    resid_hist = draw_resid_hist(jax.random.fold_in(key_list[6], 71), 0)
    return dict(psi_hat=psi_hat, occupations=occupations, weights=weights, density_in=density_in, dens_hist=dens_hist, resid_hist=resid_hist)


highest = lax.Precision.HIGHEST
beta_mix = 0.3
regular = 0.01

def dft_tables():
    indices = jnp.arange(NG, dtype=jnp.int32)
    product = indices[:, None] * indices[None, :] % NG
    angles = product.astype(jnp.float32) * jnp.float32(2.0 * 3.141592653589793 / NG)
    return (jnp.cos(angles), jnp.sin(angles))

def rotate(pattern, real_part, imag_part, cosine_table, sine_table):
    einsum = partial(jnp.einsum, precision=highest)
    out_real = einsum(pattern, real_part, cosine_table) - einsum(pattern, imag_part, sine_table)
    out_imag = einsum(pattern, real_part, sine_table) + einsum(pattern, imag_part, cosine_table)
    return (out_real, out_imag)

def band_power(coeffs, cosine_table, sine_table):
    real_part, imag_part = rotate('pqk,kz->zpq', coeffs[0], coeffs[1], cosine_table, sine_table)
    real_part, imag_part = rotate('zpq,qy->zpy', real_part, imag_part, cosine_table, sine_table)
    real_part, imag_part = rotate('zpy,px->zxy', real_part, imag_part, cosine_table, sine_table)
    return (real_part * real_part + imag_part * imag_part) * jnp.float32(1.0 / NG ** 3)

def broyden(density, density_in, dens_hist, resid_hist):
    residual_now = density - density_in
    gram = jnp.einsum('hzxy,gzxy->hg', resid_hist, resid_hist, precision=highest)
    projections = jnp.einsum('hzxy,zxy->h', resid_hist, residual_now, precision=highest)
    system = gram + regular * jnp.diag(jnp.diag(gram))
    chol_factor = jnp.linalg.cholesky(system)
    mix_coefs = jax.scipy.linalg.cho_solve((chol_factor, True), projections)
    update = jnp.einsum('h,hzxy->zxy', mix_coefs, dens_hist + beta_mix * resid_hist, precision=highest)
    return density_in + beta_mix * residual_now - update

def reference(psi_hat, occupations, weights, density_in, dens_hist, resid_hist):
    cosine_table, sine_table = dft_tables()
    weight_total = jnp.sum(weights.astype(jnp.float32))

    def per_point(point_total, point_inputs):
        coeffs_point, occ_point, weight_point = point_inputs

        def per_band(band_total, band_inputs):
            coeffs_band, occ_band = band_inputs
            power = band_power(coeffs_band, cosine_table, sine_table)
            return (band_total + occ_band.astype(jnp.float32) * power, None)
        pool_term, unused = lax.scan(per_band, jnp.zeros((NG, NG, NG), jnp.float32), (coeffs_point, occ_point))
        return (point_total + pool_term * (weight_point.astype(jnp.float32) / weight_total), None)
    density, unused = lax.scan(per_point, jnp.zeros((NG, NG, NG), jnp.float32), (psi_hat, occupations, weights))
    mixed_density = broyden(density, density_in, dens_hist, resid_hist)
    return (density, mixed_density)
```

```python
from functools import partial

import jax
import jax.numpy as jnp
import ml_dtypes
import numpy as np
from jax import lax
from jax.experimental import pallas as pl
from jax.experimental.pallas import tpu as pltpu
from jax.sharding import PartitionSpec as P

NG = 128
BANDS = 12
HIST = 8
KA = 8
NB = 32
XS = 4
PLANES = NG // NB
REST = BANDS - 1
ROWS = REST * 8
QUARTER = NG // XS
CHUNKS = PLANES + 1
BETA = 0.3
REGULAR = 0.01
MESH = pl.DeviceIdType.MESH


def split_table(table):
    high = table.astype(ml_dtypes.bfloat16)
    low = (table - high.astype(np.float64)).astype(ml_dtypes.bfloat16)
    return high, low


def dft_tables():
    index = np.arange(NG)
    angles = 2.0 * np.pi * (index[:, None] * index[None, :] % NG) / NG
    cosine, sine = np.cos(angles), np.sin(angles)
    table = np.block([[cosine, -sine], [sine, cosine]])
    order = [
        part * NG + source * PLANES + p
        for source in range(NB)
        for part in range(2)
        for p in range(PLANES)
    ]
    return (*split_table(table), *split_table(table[:, order]))


def split(x):
    high = x.astype(jnp.bfloat16)
    low = (x - high.astype(jnp.float32)).astype(jnp.bfloat16)
    return high, low


def times(table_high, table_low, x, contract):
    high, low = split(x)
    dot = partial(
        lax.dot_general,
        dimension_numbers=(((1,), (contract,)), ((), ())),
        preferred_element_type=jnp.float32,
    )
    return dot(table_high, high) + (dot(table_low, high) + dot(table_high, low))


def diagonal_row(columns):
    sums = jnp.sum(columns, axis=1, keepdims=True)
    shape = columns.shape
    on = lax.broadcasted_iota(jnp.int32, shape, 0) == lax.broadcasted_iota(jnp.int32, shape, 1)
    return jnp.sum(jnp.where(on, sums, 0.0), axis=0, keepdims=True)


def spread_rows(row, count):
    shape = (count, 128)
    on = lax.broadcasted_iota(jnp.int32, shape, 0) == lax.broadcasted_iota(jnp.int32, shape, 1)
    picked = jnp.sum(jnp.where(on, row, 0.0), axis=1, keepdims=True)
    return jnp.broadcast_to(picked, shape)


def kernel(
    occ, weights, psi, din_hbm, dens_hbm, resid_hbm, th_hbm, tl_hbm, xh_hbm, xl_hbm,
    out_density, out_mixed,
    psi_v, din, dens, resid, th, tl, xh, xl,
    send_a, send_b, recv_a, recv_b,
    plane_buf, rs_buf, z_send, z_recv, gram_part, gram_rows, proj_rows, w_rows, chol,
    psi_sem, load_sem, own_sem,
    band_send, band_recv, rs_send, rs_recv, z_ssem, z_rsem, ag_send, ag_recv,
    gram_ssem, gram_rsem, proj_ssem, proj_rsem, w_ssem, w_rsem,
):
    ka = lax.axis_index("ka")
    me = lax.axis_index("band")
    z_hi, x = lax.div(ka, XS), lax.rem(ka, XS)
    y, z, core = lax.div(me, 8), lax.rem(lax.div(me, 2), 4), lax.rem(me, 2)

    def band_peer(n):
        step = NB - 1 - n
        dz, dy, dc = lax.div(step, 8), lax.rem(lax.div(step, 2), 4), lax.rem(step, 2)
        z_top = lax.rem(lax.div(z, 2) + lax.div(dz, 2), 2)
        z_low = lax.rem(z + dz, 2)
        return lax.rem(y + dy, 4) * 8 + (z_top * 2 + z_low) * 2 + lax.rem(core + dc, 2)

    def ka_peer(n):
        return lax.rem(ka + 1 + n, KA)

    def x_peer(n):
        return lax.rem(x + 1 + n, XS)

    def each(count, body):
        def step(n, carry):
            body(n)
            return carry

        lax.fori_loop(0, count, step, 0)

    def psi_load(b):
        return pltpu.make_async_copy(psi.at[0, b], psi_v.at[b], psi_sem.at[b])

    loads = [
        pltpu.make_async_copy(src, dst, load_sem.at[i])
        for i, (src, dst) in enumerate(
            [
                (th_hbm, th), (tl_hbm, tl), (xh_hbm, xh), (xl_hbm, xl),
                (resid_hbm, resid), (dens_hbm, dens), (din_hbm, din),
            ]
        )
    ]
    loads[0].start()
    loads[1].start()
    each(BANDS, lambda b: psi_load(b).start())
    for load in loads[2:]:
        load.start()

    barrier = pltpu.get_barrier_semaphore()

    def greet_band(n):
        pl.semaphore_signal(barrier, inc=1, device_id=(ka, band_peer(n)), device_id_type=MESH)

    def greet_ka(n):
        pl.semaphore_signal(barrier, inc=1, device_id=(ka_peer(n), me), device_id_type=MESH)

    each(NB - 1, greet_band)
    each(KA - 1, greet_ka)
    loads[0].wait()
    loads[1].wait()

    def transform(b, store):
        psi_load(b).wait()
        columns = jnp.concatenate(
            [
                jnp.concatenate([psi_v[b, 0, p], psi_v[b, 1, p]], axis=0)
                for p in range(PLANES)
            ],
            axis=1,
        )
        along_y = times(th[...], tl[...], columns, 0)
        rows = jnp.concatenate(
            [
                jnp.concatenate(
                    [
                        along_y[:NG, p * NG : (p + 1) * NG],
                        along_y[NG:, p * NG : (p + 1) * NG],
                    ],
                    axis=1,
                )
                for p in range(PLANES)
            ],
            axis=0,
        )
        along_z = times(th[...], tl[...], rows, 1)
        for part in range(2):
            for p in range(PLANES):
                store(
                    part * PLANES + p,
                    along_z[part * NG : (part + 1) * NG, p * NG : (p + 1) * NG],
                )

    def store_a(j, block):
        send_a[pl.ds(j, NG, stride=8), :] = block

    transform(0, store_a)
    pl.semaphore_wait(barrier, NB + KA - 2)

    def copy_a(n, peer, slot):
        return pltpu.make_async_remote_copy(
            src_ref=send_a.at[pl.ds(peer * 32, 32), :],
            dst_ref=recv_a.at[slot],
            send_sem=band_send.at[0, n],
            recv_sem=band_recv.at[0, slot],
            device_id=(ka, peer),
            device_id_type=MESH,
        )

    def copy_b(zi, n, peer, slot):
        return pltpu.make_async_remote_copy(
            src_ref=send_b.at[pl.ds((peer * PLANES + zi) * ROWS, ROWS), :],
            dst_ref=recv_b.at[zi * NB + slot],
            send_sem=band_send.at[zi + 1, n],
            recv_sem=band_recv.at[zi + 1, slot],
            device_id=(ka, peer),
            device_id_type=MESH,
        )

    def own_b(zi):
        return pltpu.make_async_copy(
            send_b.at[pl.ds((me * PLANES + zi) * ROWS, ROWS), :],
            recv_b.at[zi * NB + me],
            own_sem.at[zi + 1],
        )

    own_a = pltpu.make_async_copy(
        send_a.at[pl.ds(me * 32, 32), :], recv_a.at[me], own_sem.at[0]
    )

    each(NB - 1, lambda n: copy_a(n, band_peer(n), me).start())
    own_a.start()

    def store_b(b):
        def store(j, block):
            send_b[pl.ds((b - 1) * 8 + j, NG, stride=ROWS), :] = block

        return store

    each(REST, lambda i: transform(i + 1, store_b(i + 1)))

    def start_b(zi):
        each(NB - 1, lambda n: copy_b(zi, n, band_peer(n), me).start())
        own_b(zi).start()

    start_b(0)

    own_weight = jnp.full((1, 128), weights[0].astype(jnp.float32))
    w_rows[ka] = own_weight

    def w_copy(n, peer, slot):
        return pltpu.make_async_remote_copy(
            src_ref=w_rows.at[ka],
            dst_ref=w_rows.at[slot],
            send_sem=w_ssem.at[n],
            recv_sem=w_rsem.at[slot],
            device_id=(peer, me),
            device_id_type=MESH,
        )

    loads[4].wait()

    def gram_step(h):
        product = resid[h].reshape(1, PLANES * NG // 8, 8, NG) * resid[...].reshape(
            HIST, PLANES * NG // 8, 8, NG
        )
        gram_part[pl.ds(pl.multiple_of(h * HIST, HIST), HIST), :] = jnp.sum(
            jnp.sum(product, axis=1), axis=1
        )

    each(HIST, gram_step)
    each(KA - 1, lambda n: w_copy(n, ka_peer(n), ka).start())
    gram_rows[me] = diagonal_row(gram_part[...])

    def row_copy(rows, ssem, rsem, n, peer, slot):
        return pltpu.make_async_remote_copy(
            src_ref=rows.at[me],
            dst_ref=rows.at[slot],
            send_sem=ssem.at[n],
            recv_sem=rsem.at[slot],
            device_id=(ka, peer),
            device_id_type=MESH,
        )

    loads[5].wait()
    loads[6].wait()
    dens[...] = dens[...] + BETA * resid[...]

    start_b(1)
    gram_copy = partial(row_copy, gram_rows, gram_ssem, gram_rsem)
    each(NB - 1, lambda n: gram_copy(n, band_peer(n), me).start())

    each(KA - 1, lambda n: w_copy(n, ka_peer(n), ka_peer(n)).wait_recv())
    total_weight = jnp.sum(w_rows[...], axis=0)
    factor = own_weight / total_weight * jnp.float32(1.0 / NG**3)

    loads[2].wait()
    loads[3].wait()

    def operand_a(zi):
        return recv_a[:, pl.ds(pl.multiple_of(zi * 8, 8), 8), :].reshape(2 * NG, NG)

    def operand_b(zi, b):
        return recv_b[
            pl.ds(zi * NB, NB), pl.ds(pl.multiple_of((b - 1) * 8, 8), 8), :
        ].reshape(2 * NG, NG)

    def pair_power(left, right, b_left, b_right):
        field = times(xh[...], xl[...], jnp.concatenate([left, right], axis=1), 0)
        power = field[:NG] * field[:NG] + field[NG:] * field[NG:]
        return (
            power[:, :NG] * occ[0, b_left].astype(jnp.float32)
            + power[:, NG:] * occ[0, b_right].astype(jnp.float32)
        )

    def compute_plane(zi):
        plane_buf[zi] = pair_power(operand_a(zi), operand_b(zi, REST), 0, REST)

        def pair(i):
            b = 2 * i + 1
            plane_buf[zi] = plane_buf[zi] + pair_power(
                operand_b(zi, b), operand_b(zi, b + 1), b, b + 1
            )

        each(REST // 2, pair)
        plane_buf[zi] = plane_buf[zi] * factor

    def rs_copy(zi, n, peer, slot):
        return pltpu.make_async_remote_copy(
            src_ref=plane_buf.at[zi, pl.ds(peer * QUARTER, QUARTER), :],
            dst_ref=rs_buf.at[zi, slot],
            send_sem=rs_send.at[zi, n],
            recv_sem=rs_recv.at[zi, slot],
            device_id=(z_hi * XS + peer, me),
            device_id_type=MESH,
        )

    def z_copy(zi):
        return pltpu.make_async_remote_copy(
            src_ref=z_send.at[zi],
            dst_ref=z_recv.at[zi],
            send_sem=z_ssem.at[zi],
            recv_sem=z_rsem.at[zi],
            device_id=(lax.rem(ka + XS, KA), me),
            device_id_type=MESH,
        )

    def ag_copy(zi, n, peer, slot):
        mine = pl.ds(pl.multiple_of(x * QUARTER, QUARTER), QUARTER)
        return pltpu.make_async_remote_copy(
            src_ref=out_density.at[zi, mine, :],
            dst_ref=out_density.at[zi, mine, :],
            send_sem=ag_send.at[zi, n],
            recv_sem=ag_recv.at[zi, slot],
            device_id=(z_hi * XS + peer, me),
            device_id_type=MESH,
        )

    def gather_start(zi):
        z_copy(zi).wait_recv()
        mine = pl.ds(pl.multiple_of(x * QUARTER, QUARTER), QUARTER)
        out_density[zi, mine, :] = z_send[zi] + z_recv[zi]
        each(XS - 1, lambda n: ag_copy(zi, n, x_peer(n), x).start())

    def plane_step(zi):
        def arrived(n):
            peer = band_peer(n)
            copy_b(zi, n, peer, peer).wait_recv()

        each(NB - 1, arrived)
        own_b(zi).wait()
        compute_plane(zi)
        each(XS - 1, lambda n: rs_copy(zi, n, x_peer(n), x).start())

    def plane_finish(zi):
        each(XS - 1, lambda n: rs_copy(zi, n, x_peer(n), x_peer(n)).wait_recv())
        mine = pl.ds(pl.multiple_of(x * QUARTER, QUARTER), QUARTER)
        z_send[zi] = (
            plane_buf[zi, mine, :]
            + rs_buf[zi, lax.rem(x + 1, XS)]
            + rs_buf[zi, lax.rem(x + 2, XS)]
            + rs_buf[zi, lax.rem(x + 3, XS)]
        )
        z_copy(zi).start()

    def arrived_a(n):
        peer = band_peer(n)
        copy_a(n, peer, peer).wait_recv()

    each(NB - 1, arrived_a)
    own_a.wait()

    def early(zi):
        plane_step(zi)

        @pl.when(zi < PLANES - 2)
        def _():
            start_b(zi + 2)

        @pl.when(zi < PLANES - 1)
        def _():
            plane_finish(zi)

        @pl.when(zi == 1)
        def _():
            factorize()

    def factorize():
        each(NB - 1, lambda n: gram_copy(n, band_peer(n), band_peer(n)).wait_recv())
        gram_part[...] = spread_rows(jnp.sum(gram_rows[...], axis=0), HIST * HIST)

        def entry(i, j):
            return gram_part[i * HIST + j : i * HIST + j + 1, :]

        lower = {}
        for j in range(HIST):
            pivot = entry(j, j) * (1.0 + REGULAR)
            for k in range(j):
                pivot = pivot - lower[j, k] * lower[j, k]
            inverse = 1.0 / jnp.sqrt(pivot)
            chol[j * HIST + j : j * HIST + j + 1, :] = inverse
            for i in range(j + 1, HIST):
                value = entry(i, j)
                for k in range(j):
                    value = value - lower[i, k] * lower[j, k]
                lower[i, j] = value * inverse
                chol[i * HIST + j : i * HIST + j + 1, :] = lower[i, j]

    each(PLANES, early)

    last = PLANES - 1
    each(last, gather_start)
    plane_finish(last)
    gather_start(last)

    def gathered(zi):
        each(XS - 1, lambda n: ag_copy(zi, n, x_peer(n), x_peer(n)).wait_recv())

    each(PLANES, gathered)

    residual = out_density[...] - din[...]
    product = (resid[...] * residual[None]).reshape(HIST, PLANES * NG // 8, 8, NG)
    proj_rows[me] = diagonal_row(jnp.sum(jnp.sum(product, axis=1), axis=1))
    proj_copy = partial(row_copy, proj_rows, proj_ssem, proj_rsem)
    each(NB - 1, lambda n: proj_copy(n, band_peer(n), me).start())
    each(NB - 1, lambda n: proj_copy(n, band_peer(n), band_peer(n)).wait_recv())
    right = spread_rows(jnp.sum(proj_rows[...], axis=0), HIST)

    def factor_entry(i, j):
        return chol[i * HIST + j : i * HIST + j + 1, :]

    forward = []
    for i in range(HIST):
        value = right[i : i + 1, :]
        for j in range(i):
            value = value - factor_entry(i, j) * forward[j]
        forward.append(value * factor_entry(i, i))
    coefs = [None] * HIST
    for i in reversed(range(HIST)):
        value = forward[i]
        for j in range(i + 1, HIST):
            value = value - factor_entry(j, i) * coefs[j]
        coefs[i] = value * factor_entry(i, i)

    for zi in range(PLANES):
        mixed = din[zi] + BETA * (out_density[zi] - din[zi])
        update = coefs[0] * dens[0, zi]
        for h in range(1, HIST):
            update = update + coefs[h] * dens[h, zi]
        out_mixed[zi] = mixed - update

    each(NB - 1, lambda n: copy_a(n, band_peer(n), me).wait_send())
    each(
        PLANES,
        lambda zi: each(NB - 1, lambda n: copy_b(zi, n, band_peer(n), me).wait_send()),
    )
    each(NB - 1, lambda n: gram_copy(n, band_peer(n), me).wait_send())
    each(NB - 1, lambda n: proj_copy(n, band_peer(n), me).wait_send())
    each(KA - 1, lambda n: w_copy(n, ka_peer(n), ka).wait_send())

    def sent(zi):
        each(XS - 1, lambda n: rs_copy(zi, n, x_peer(n), x).wait_send())
        z_copy(zi).wait_send()
        each(XS - 1, lambda n: ag_copy(zi, n, x_peer(n), x).wait_send())

    each(PLANES, sent)


def shards(psi_hat, occupations, weights, density_in, dens_hist, resid_hist):
    th, tl, xh, xl = (jnp.asarray(table) for table in dft_tables())
    plane = (PLANES, NG, NG)
    f32 = jnp.float32
    dma = pltpu.SemaphoreType.DMA
    vmem = partial(pltpu.VMEM)
    any_spec = pl.BlockSpec(memory_space=pl.ANY)
    smem_spec = pl.BlockSpec(memory_space=pltpu.SMEM)
    vmem_spec = pl.BlockSpec(memory_space=pltpu.VMEM)
    table = vmem((2 * NG, 2 * NG), jnp.bfloat16)
    return pl.pallas_call(
        kernel,
        out_shape=(jax.ShapeDtypeStruct(plane, f32), jax.ShapeDtypeStruct(plane, f32)),
        in_specs=[smem_spec, smem_spec] + [any_spec] * 8,
        out_specs=(vmem_spec, vmem_spec),
        scratch_shapes=[
            vmem((BANDS, 2, PLANES, NG, NG), f32),
            vmem(plane, f32),
            vmem((HIST, *plane), f32),
            vmem((HIST, *plane), f32),
            table, table, table, table,
            vmem((NG * 8, NG), f32),
            vmem((NG * ROWS, NG), f32),
            vmem((NB, 8 * PLANES, NG), f32),
            vmem((PLANES * NB, ROWS, NG), f32),
            vmem(plane, f32),
            vmem((PLANES, XS, QUARTER, NG), f32),
            vmem((PLANES, QUARTER, NG), f32),
            vmem((PLANES, QUARTER, NG), f32),
            vmem((HIST * HIST, 128), f32),
            vmem((NB, 1, 128), f32),
            vmem((NB, 1, 128), f32),
            vmem((KA, 1, 128), f32),
            vmem((HIST * HIST, 128), f32),
            dma((BANDS,)), dma((7,)), dma((CHUNKS,)),
            dma((CHUNKS, NB)), dma((CHUNKS, NB)),
            dma((PLANES, XS)), dma((PLANES, XS)),
            dma((PLANES,)), dma((PLANES,)),
            dma((PLANES, XS)), dma((PLANES, XS)),
            dma((NB,)), dma((NB,)), dma((NB,)), dma((NB,)),
            dma((KA,)), dma((KA,)),
        ],
        compiler_params=pltpu.CompilerParams(
            collective_id=0, has_side_effects=True, vmem_limit_bytes=56 * 1024 * 1024
        ),
    )(occupations, weights, psi_hat, density_in, dens_hist, resid_hist, th, tl, xh, xl)


def solution(mesh):
    return jax.shard_map(
        shards,
        mesh=mesh,
        in_specs=(
            P("ka", None, None, "band", None, None),
            P("ka", None),
            P("ka"),
            P("band", None, None),
            P(None, "band", None, None),
            P(None, "band", None, None),
        ),
        out_specs=(P("band", None, None), P("band", None, None)),
        check_vma=False,
    )
```

```python
from functools import partial

import jax
import jax.numpy as jnp
import ml_dtypes
import numpy as np
from jax import lax
from jax.experimental import pallas as pl
from jax.experimental.pallas import tpu as pltpu
from jax.sharding import PartitionSpec as P

NG = 128
BANDS = 12
HIST = 8
KA = 8
NB = 32
XS = 4
PLANES = NG // NB
REST = BANDS - 1
ROWS = REST * 8
QUARTER = NG // XS
CHUNKS = PLANES + 1
BETA = 0.3
REGULAR = 0.01
MESH = pl.DeviceIdType.MESH


def split_table(table):
    high = table.astype(ml_dtypes.bfloat16)
    low = (table - high.astype(np.float64)).astype(ml_dtypes.bfloat16)
    return high, low


def dft_tables():
    index = np.arange(NG)
    angles = 2.0 * np.pi * (index[:, None] * index[None, :] % NG) / NG
    cosine, sine = np.cos(angles), np.sin(angles)
    table = np.block([[cosine, -sine], [sine, cosine]])
    order = [
        part * NG + source * PLANES + p
        for source in range(NB)
        for part in range(2)
        for p in range(PLANES)
    ]
    return (*split_table(table), *split_table(table[:, order]))


def split(x):
    high = x.astype(jnp.bfloat16)
    low = (x - high.astype(jnp.float32)).astype(jnp.bfloat16)
    return high, low


def times(table_high, table_low, x, contract):
    high, low = split(x)
    dot = partial(
        lax.dot_general,
        dimension_numbers=(((1,), (contract,)), ((), ())),
        preferred_element_type=jnp.float32,
    )
    return dot(table_high, high) + (dot(table_low, high) + dot(table_high, low))


def diagonal_row(columns):
    sums = jnp.sum(columns, axis=1, keepdims=True)
    shape = columns.shape
    on = lax.broadcasted_iota(jnp.int32, shape, 0) == lax.broadcasted_iota(jnp.int32, shape, 1)
    return jnp.sum(jnp.where(on, sums, 0.0), axis=0, keepdims=True)


def spread_rows(row, count):
    shape = (count, 128)
    on = lax.broadcasted_iota(jnp.int32, shape, 0) == lax.broadcasted_iota(jnp.int32, shape, 1)
    picked = jnp.sum(jnp.where(on, row, 0.0), axis=1, keepdims=True)
    return jnp.broadcast_to(picked, shape)


def kernel(
    weights, occ_hbm, psi, din_hbm, dens_hbm, resid_hbm, th_hbm, tl_hbm, xh_hbm, xl_hbm,
    out_density, out_mixed,
    occ, psi_v, din, dens, resid, th, tl, xh, xl,
    send_a, send_b, recv_a, recv_b,
    plane_buf, rs_buf, z_send, z_recv, gram_part, gram_rows, proj_part, proj_rows, total_rows, w_rows, inverse,
    psi_sem, load_sem, own_sem,
    band_send, band_recv, rs_send, rs_recv, z_ssem, z_rsem, ag_send, ag_recv,
    gram_sem, proj_sem, total_sem, w_sem,
):
    ka = lax.axis_index("ka")
    me = lax.axis_index("band")
    z_hi, x = lax.div(ka, XS), lax.rem(ka, XS)
    y, z, core = lax.div(me, 8), lax.rem(lax.div(me, 2), 4), lax.rem(me, 2)

    def band_peer(n):
        step = NB - 1 - n
        dz, dy, dc = lax.div(step, 8), lax.rem(lax.div(step, 2), 4), lax.rem(step, 2)
        z_top = lax.rem(lax.div(z, 2) + lax.div(dz, 2), 2)
        z_low = lax.rem(z + dz, 2)
        return lax.rem(y + dy, 4) * 8 + (z_top * 2 + z_low) * 2 + lax.rem(core + dc, 2)

    def ka_peer(n):
        return lax.rem(ka + 1 + n, KA)

    def x_peer(n):
        return lax.rem(x + 1 + n, XS)

    def each(count, body):
        def step(n, carry):
            body(n)
            return carry

        lax.fori_loop(0, count, step, 0)

    def wait_bytes(ref, sem):
        pltpu.make_async_copy(ref, ref, sem).wait()

    mine = pl.ds(pl.multiple_of(x * QUARTER, QUARTER), QUARTER)

    barrier = pltpu.get_barrier_semaphore()

    def greet_band(n):
        pl.semaphore_signal(barrier, inc=1, device_id=(ka, band_peer(n)), device_id_type=MESH)

    def greet_ka(n):
        pl.semaphore_signal(barrier, inc=1, device_id=(ka_peer(n), me), device_id_type=MESH)

    each(NB - 1, greet_band)
    each(KA - 1, greet_ka)

    first_psi = pltpu.make_async_copy(psi.at[0, 0], psi_v.at[0], psi_sem.at[0])
    other_psi = pltpu.make_async_copy(
        psi.at[0, pl.ds(1, REST)], psi_v.at[pl.ds(1, REST)], psi_sem.at[1]
    )
    loads = [
        pltpu.make_async_copy(src, dst, load_sem.at[i])
        for i, (src, dst) in enumerate(
            [
                (th_hbm, th), (tl_hbm, tl), (xh_hbm, xh), (xl_hbm, xl),
                (resid_hbm, resid), (dens_hbm, dens), (din_hbm, din),
                (occ_hbm, occ),
            ]
        )
    ]
    loads[0].start()
    loads[1].start()
    first_psi.start()
    other_psi.start()
    for load in loads[2:]:
        load.start()
    loads[0].wait()
    loads[1].wait()
    first_psi.wait()

    def transform(b, store):
        columns = jnp.concatenate(
            [
                jnp.concatenate([psi_v[b, 0, p], psi_v[b, 1, p]], axis=0)
                for p in range(PLANES)
            ],
            axis=1,
        )
        along_y = times(th[...], tl[...], columns, 0)
        rows = jnp.concatenate(
            [
                jnp.concatenate(
                    [
                        along_y[:NG, p * NG : (p + 1) * NG],
                        along_y[NG:, p * NG : (p + 1) * NG],
                    ],
                    axis=1,
                )
                for p in range(PLANES)
            ],
            axis=0,
        )
        along_z = times(th[...], tl[...], rows, 1)
        for part in range(2):
            for p in range(PLANES):
                store(
                    part * PLANES + p,
                    along_z[part * NG : (part + 1) * NG, p * NG : (p + 1) * NG],
                )

    def store_a(j, block):
        send_a[pl.ds(j, NG, stride=8), :] = block

    transform(0, store_a)
    pl.semaphore_wait(barrier, NB + KA - 2)

    def start_a(n):
        peer = band_peer(n)
        pltpu.make_async_remote_copy(
            src_ref=send_a.at[pl.ds(peer * 32, 32), :],
            dst_ref=recv_a.at[me],
            send_sem=band_send.at[0],
            recv_sem=band_recv.at[0],
            device_id=(ka, peer),
            device_id_type=MESH,
        ).start()

    own_a = pltpu.make_async_copy(
        send_a.at[pl.ds(me * 32, 32), :], recv_a.at[me], own_sem.at[0]
    )

    def own_b(zi):
        return pltpu.make_async_copy(
            send_b.at[pl.ds((me * PLANES + zi) * ROWS, ROWS), :],
            recv_b.at[zi * NB + me],
            own_sem.at[zi + 1],
        )

    def start_b(zi):
        def start(n):
            peer = band_peer(n)
            pltpu.make_async_remote_copy(
                src_ref=send_b.at[pl.ds((peer * PLANES + zi) * ROWS, ROWS), :],
                dst_ref=recv_b.at[zi * NB + me],
                send_sem=band_send.at[zi + 1],
                recv_sem=band_recv.at[zi + 1],
                device_id=(ka, peer),
                device_id_type=MESH,
            ).start()

        each(NB - 1, start)
        own_b(zi).start()

    def wait_b(zi, sems):
        wait_bytes(recv_b.at[pl.ds(zi * NB, NB - 1)], sems.at[zi + 1])

    def start_row(rows, sem, peer):
        pltpu.make_async_remote_copy(
            src_ref=rows.at[me],
            dst_ref=rows.at[me],
            send_sem=sem.at[0],
            recv_sem=sem.at[1],
            device_id=(ka, peer),
            device_id_type=MESH,
        ).start()

    def start_ka_row(rows, sem, peer):
        pltpu.make_async_remote_copy(
            src_ref=rows.at[ka],
            dst_ref=rows.at[ka],
            send_sem=sem.at[0],
            recv_sem=sem.at[1],
            device_id=(peer, me),
            device_id_type=MESH,
        ).start()

    def wait_rows(rows, count, sem, side):
        wait_bytes(rows.at[pl.ds(0, count - 1)], sem.at[side])

    each(NB - 1, start_a)
    own_a.start()

    def store_b(b):
        def store(j, block):
            send_b[pl.ds((b - 1) * 8 + j, NG, stride=ROWS), :] = block

        return store

    other_psi.wait()
    each(REST, lambda i: transform(i + 1, store_b(i + 1)))
    loads[7].wait()
    own_weight = jnp.full((1, 128), weights[0].astype(jnp.float32))
    w_rows[ka] = own_weight
    start_b(0)

    loads[4].wait()

    def gram_step(h):
        product = resid[h].reshape(1, PLANES * NG // 8, 8, NG) * resid[...].reshape(
            HIST, PLANES * NG // 8, 8, NG
        )
        gram_part[pl.ds(pl.multiple_of(h * HIST, HIST), HIST), :] = jnp.sum(
            jnp.sum(product, axis=1), axis=1
        )

    each(HIST, gram_step)
    each(KA - 1, lambda n: start_ka_row(w_rows, w_sem, ka_peer(n)))
    gram_rows[me] = diagonal_row(gram_part[...])

    loads[5].wait()
    loads[6].wait()
    dens[...] = dens[...] + BETA * resid[...]
    proj_part[...] = jnp.zeros((HIST, 128), jnp.float32)

    start_b(1)
    each(NB - 1, lambda n: start_row(gram_rows, gram_sem, band_peer(n)))

    wait_rows(w_rows, KA, w_sem, 1)
    factor = own_weight / jnp.sum(w_rows[...], axis=0) * jnp.float32(1.0 / NG**3)
    loads[2].wait()
    loads[3].wait()

    def operand_a(zi):
        return recv_a[:, pl.ds(pl.multiple_of(zi * 8, 8), 8), :].reshape(2 * NG, NG)

    def operand_b(zi, b):
        return recv_b[
            pl.ds(zi * NB, NB), pl.ds(pl.multiple_of((b - 1) * 8, 8), 8), :
        ].reshape(2 * NG, NG)

    def pair_power(left, right, b_left, b_right):
        field = times(xh[...], xl[...], jnp.concatenate([left, right], axis=1), 0)
        power = field[:NG] * field[:NG] + field[NG:] * field[NG:]
        return (
            power[:, :NG] * occ[0, b_left].astype(jnp.float32)
            + power[:, NG:] * occ[0, b_right].astype(jnp.float32)
        )

    def compute_plane(zi):
        plane_buf[zi] = pair_power(operand_a(zi), operand_b(zi, REST), 0, REST)

        def pair(i):
            b = 2 * i + 1
            plane_buf[zi] = plane_buf[zi] + pair_power(
                operand_b(zi, b), operand_b(zi, b + 1), b, b + 1
            )

        each(REST // 2, pair)
        plane_buf[zi] = plane_buf[zi] * factor

    def start_rs(zi):
        def start(n):
            peer = x_peer(n)
            pltpu.make_async_remote_copy(
                src_ref=plane_buf.at[zi, pl.ds(peer * QUARTER, QUARTER), :],
                dst_ref=rs_buf.at[zi, x],
                send_sem=rs_send.at[zi],
                recv_sem=rs_recv.at[zi],
                device_id=(z_hi * XS + peer, me),
                device_id_type=MESH,
            ).start()

        each(XS - 1, start)

    def z_copy(zi):
        return pltpu.make_async_remote_copy(
            src_ref=z_send.at[zi],
            dst_ref=z_recv.at[zi],
            send_sem=z_ssem.at[zi],
            recv_sem=z_rsem.at[zi],
            device_id=(lax.rem(ka + XS, KA), me),
            device_id_type=MESH,
        )

    def add_up(zi):
        wait_bytes(rs_buf.at[zi, pl.ds(0, XS - 1)], rs_recv.at[zi])
        z_send[zi] = (
            plane_buf[zi, mine, :]
            + rs_buf[zi, lax.rem(x + 1, XS)]
            + rs_buf[zi, lax.rem(x + 2, XS)]
            + rs_buf[zi, lax.rem(x + 3, XS)]
        )
        z_copy(zi).start()

    def start_gather(zi):
        z_copy(zi).wait_recv()
        out_density[zi, mine, :] = z_send[zi] + z_recv[zi]

        def start(n):
            pltpu.make_async_remote_copy(
                src_ref=out_density.at[zi, mine, :],
                dst_ref=out_density.at[zi, mine, :],
                send_sem=ag_send.at[zi],
                recv_sem=ag_recv.at[zi],
                device_id=(z_hi * XS + x_peer(n), me),
                device_id_type=MESH,
            ).start()

        each(XS - 1, start)

    def project(zi):
        own = plane_buf[zi] - (1.0 / KA) * din[zi]
        product = (resid[:, zi] * own[None]).reshape(HIST, NG // 8, 8, NG)
        proj_part[...] = proj_part[...] + jnp.sum(jnp.sum(product, axis=1), axis=1)

    def plane_step(zi):
        wait_b(zi, band_recv)
        own_b(zi).wait()
        compute_plane(zi)
        start_rs(zi)
        project(zi)

    def invert():
        wait_rows(gram_rows, NB, gram_sem, 1)
        gram_part[...] = spread_rows(jnp.sum(gram_rows[...], axis=0), HIST * HIST)

        def entry(i, j):
            return gram_part[i * HIST + j : i * HIST + j + 1, :]

        lower, pivots = {}, []
        for j in range(HIST):
            pivot = entry(j, j) * (1.0 + REGULAR)
            for k in range(j):
                pivot = pivot - lower[j, k] * lower[j, k]
            pivots.append(1.0 / jnp.sqrt(pivot))
            for i in range(j + 1, HIST):
                value = entry(i, j)
                for k in range(j):
                    value = value - lower[i, k] * lower[j, k]
                lower[i, j] = value * pivots[j]
        unlower = {}
        for j in range(HIST):
            unlower[j, j] = pivots[j]
            for i in range(j + 1, HIST):
                value = lower[i, j] * unlower[j, j]
                for k in range(j + 1, i):
                    value = value + lower[i, k] * unlower[k, j]
                unlower[i, j] = -value * pivots[i]
        lane = lax.broadcasted_iota(jnp.int32, (1, 128), 1)
        for i in range(HIST):
            row = jnp.zeros((1, 128), jnp.float32)
            for j in range(HIST):
                value = sum(unlower[k, i] * unlower[k, j] for k in range(max(i, j), HIST))
                row = jnp.where(lane == j, value, row)
            inverse[i : i + 1, :] = row

    def early(zi):
        plane_step(zi)
        add_up(zi)

        @pl.when(zi < PLANES - 2)
        def _():
            start_b(zi + 2)

        @pl.when(zi > 0)
        def _():
            start_gather(zi - 1)

        @pl.when(zi == 1)
        def _():
            invert()

    last = PLANES - 1
    wait_bytes(recv_a.at[pl.ds(0, NB - 1)], band_recv.at[0])
    own_a.wait()
    each(last, early)

    wait_bytes(recv_a.at[pl.ds(0, NB - 1)], band_send.at[0])
    for zi in range(PLANES - 2):
        wait_b(zi, band_send)
    wait_rows(w_rows, KA, w_sem, 0)
    wait_rows(gram_rows, NB, gram_sem, 0)

    plane_step(last)
    proj_rows[me] = diagonal_row(proj_part[...])
    each(NB - 1, lambda n: start_row(proj_rows, proj_sem, band_peer(n)))
    add_up(last)
    start_gather(last - 1)
    wait_rows(proj_rows, NB, proj_sem, 1)
    total_rows[ka] = jnp.sum(proj_rows[...], axis=0)
    each(KA - 1, lambda n: start_ka_row(total_rows, total_sem, ka_peer(n)))
    start_gather(last)

    for zi in range(PLANES - 2, PLANES):
        wait_b(zi, band_send)
    wait_rows(proj_rows, NB, proj_sem, 0)
    for zi in range(PLANES):
        wait_bytes(rs_buf.at[zi, pl.ds(0, XS - 1)], rs_send.at[zi])
        z_copy(zi).wait_send()

    wait_rows(total_rows, KA, total_sem, 1)
    projections = jnp.sum(total_rows[...], axis=0)
    coefs = jnp.sum(inverse[...] * projections, axis=1, keepdims=True)
    for zi in range(PLANES):
        wait_bytes(out_density.at[zi, pl.ds(0, NG - QUARTER), :], ag_recv.at[zi])
        update = coefs[0:1] * dens[0, zi]
        for h in range(1, HIST):
            update = update + coefs[h : h + 1] * dens[h, zi]
        out_mixed[zi] = din[zi] + BETA * (out_density[zi] - din[zi]) - update

    wait_rows(total_rows, KA, total_sem, 0)
    for zi in range(PLANES):
        wait_bytes(out_density.at[zi, pl.ds(0, NG - QUARTER), :], ag_send.at[zi])


def shards(psi_hat, occupations, weights, density_in, dens_hist, resid_hist):
    operands = (occupations, psi_hat, density_in, dens_hist, resid_hist)
    operands += tuple(jnp.asarray(table) for table in dft_tables())
    plane = (PLANES, NG, NG)
    f32 = jnp.float32
    dma = pltpu.SemaphoreType.DMA
    vmem = partial(pltpu.VMEM)
    hbm_spec = pl.BlockSpec(memory_space=pltpu.HBM)
    vmem_spec = pl.BlockSpec(memory_space=pltpu.VMEM)
    table = vmem((2 * NG, 2 * NG), jnp.bfloat16)
    return pl.pallas_call(
        kernel,
        out_shape=(jax.ShapeDtypeStruct(plane, f32), jax.ShapeDtypeStruct(plane, f32)),
        in_specs=[pl.BlockSpec(memory_space=pltpu.SMEM)] + [hbm_spec] * 9,
        out_specs=(vmem_spec, vmem_spec),
        scratch_shapes=[
            pltpu.SMEM((1, BANDS), jnp.int32),
            vmem((BANDS, 2, PLANES, NG, NG), f32),
            vmem(plane, f32),
            vmem((HIST, *plane), f32),
            vmem((HIST, *plane), f32),
            table, table, table, table,
            vmem((NG * 8, NG), f32),
            vmem((NG * ROWS, NG), f32),
            vmem((NB, 8 * PLANES, NG), f32),
            vmem((PLANES * NB, ROWS, NG), f32),
            vmem(plane, f32),
            vmem((PLANES, XS, QUARTER, NG), f32),
            vmem((PLANES, QUARTER, NG), f32),
            vmem((PLANES, QUARTER, NG), f32),
            vmem((HIST * HIST, 128), f32),
            vmem((NB, 1, 128), f32),
            vmem((HIST, 128), f32),
            vmem((NB, 1, 128), f32),
            vmem((KA, 1, 128), f32),
            vmem((KA, 1, 128), f32),
            vmem((HIST, 128), f32),
            dma((2,)), dma((8,)), dma((CHUNKS,)),
            dma((CHUNKS,)), dma((CHUNKS,)),
            dma((PLANES,)), dma((PLANES,)),
            dma((PLANES,)), dma((PLANES,)),
            dma((PLANES,)), dma((PLANES,)),
            dma((2,)), dma((2,)), dma((2,)), dma((2,)),
        ],
        compiler_params=pltpu.CompilerParams(
            collective_id=0, has_side_effects=True, vmem_limit_bytes=32 * 1024 * 1024
        ),
    )(weights, *(pltpu.with_memory_space_constraint(operand, pltpu.HBM) for operand in operands))


def solution(mesh):
    return jax.shard_map(
        shards,
        mesh=mesh,
        in_specs=(
            P("ka", None, None, "band", None, None),
            P("ka", None),
            P("ka"),
            P("band", None, None),
            P(None, "band", None, None),
            P(None, "band", None, None),
        ),
        out_specs=(P("band", None, None), P("band", None, None)),
        check_vma=False,
    )
```

```python
from functools import partial

import jax
import jax.numpy as jnp
import ml_dtypes
import numpy as np
from jax import lax
from jax.experimental import pallas as pl
from jax.experimental.pallas import tpu as pltpu
from jax.sharding import PartitionSpec as P

NG = 128
BANDS = 12
HIST = 8
KA = 8
NB = 32
XS = 4
PLANES = NG // NB
REST = BANDS - 1
ROWS = REST * 8
QUARTER = NG // XS
LATE = 3
CHUNKS = PLANES + 2
BETA = 0.3
REGULAR = 0.01
MESH = pl.DeviceIdType.MESH


def split_table(table):
    high = table.astype(ml_dtypes.bfloat16)
    low = (table - high.astype(np.float64)).astype(ml_dtypes.bfloat16)
    return high, low


def dft_tables():
    index = np.arange(NG)
    angles = 2.0 * np.pi * (index[:, None] * index[None, :] % NG) / NG
    cosine, sine = np.cos(angles), np.sin(angles)
    table = np.block([[cosine, -sine], [sine, cosine]])
    order = [
        part * NG + source * PLANES + p
        for source in range(NB)
        for part in range(2)
        for p in range(PLANES)
    ]
    return (*split_table(table), *split_table(table[:, order]))


def split(x):
    high = x.astype(jnp.bfloat16)
    low = (x - high.astype(jnp.float32)).astype(jnp.bfloat16)
    return high, low


def times(table_high, table_low, x, contract):
    high, low = split(x)
    dot = partial(
        lax.dot_general,
        dimension_numbers=(((1,), (contract,)), ((), ())),
        preferred_element_type=jnp.float32,
    )
    return dot(table_high, high) + (dot(table_low, high) + dot(table_high, low))


def diagonal_row(columns):
    sums = jnp.sum(columns, axis=1, keepdims=True)
    shape = columns.shape
    on = lax.broadcasted_iota(jnp.int32, shape, 0) == lax.broadcasted_iota(jnp.int32, shape, 1)
    return jnp.sum(jnp.where(on, sums, 0.0), axis=0, keepdims=True)


def spread_rows(row, count):
    shape = (count, 128)
    on = lax.broadcasted_iota(jnp.int32, shape, 0) == lax.broadcasted_iota(jnp.int32, shape, 1)
    picked = jnp.sum(jnp.where(on, row, 0.0), axis=1, keepdims=True)
    return jnp.broadcast_to(picked, shape)


def kernel(
    weights, occ_hbm, psi, din_hbm, dens_hbm, resid_hbm, th_hbm, tl_hbm, xh_hbm, xl_hbm,
    out_density, out_mixed,
    occ, psi_v, din, dens, resid, th, tl, xh, xl,
    send_a, send_b, recv_a, recv_b,
    plane_buf, rs_buf, z_send, z_recv, gram_part, gram_rows, proj_part, proj_rows, total_rows, w_rows, inverse,
    psi_sem, load_sem, own_sem,
    band_send, band_recv, rs_send, rs_recv, z_ssem, z_rsem, ag_send, ag_recv,
    gram_sem, proj_sem, total_sem, w_sem,
):
    ka = lax.axis_index("ka")
    me = lax.axis_index("band")
    z_hi, x = lax.div(ka, XS), lax.rem(ka, XS)
    y, z, core = lax.div(me, 8), lax.rem(lax.div(me, 2), 4), lax.rem(me, 2)

    def band_peer(n):
        step = NB - 1 - n
        dz, dy, dc = lax.div(step, 8), lax.rem(lax.div(step, 2), 4), lax.rem(step, 2)
        z_top = lax.rem(lax.div(z, 2) + lax.div(dz, 2), 2)
        z_low = lax.rem(z + dz, 2)
        return lax.rem(y + dy, 4) * 8 + (z_top * 2 + z_low) * 2 + lax.rem(core + dc, 2)

    y_part = [lax.rem(y + dy, 4) * 8 for dy in range(4)]
    z_part = [
        lax.rem(lax.div(z, 2) + dz // 2, 2) * 4 + lax.rem(z + dz, 2) * 2 for dz in range(4)
    ]
    core_part = [core, 1 - core]
    band_peers = [
        y_part[step // 2 % 4] + z_part[step // 8] + core_part[step % 2]
        for step in range(NB - 1, 0, -1)
    ]

    def ka_peer(n):
        return lax.rem(ka + 1 + n, KA)

    def x_peer(n):
        return lax.rem(x + 1 + n, XS)

    def each(count, body):
        def step(n, carry):
            body(n)
            return carry

        lax.fori_loop(0, count, step, 0)

    def wait_bytes(ref, sem):
        pltpu.make_async_copy(ref, ref, sem).wait()

    last = PLANES - 1
    mine = pl.ds(pl.multiple_of(x * QUARTER, QUARTER), QUARTER)

    first_psi = pltpu.make_async_copy(psi.at[0, 0], psi_v.at[0], psi_sem.at[0])
    other_psi = pltpu.make_async_copy(
        psi.at[0, pl.ds(1, REST)], psi_v.at[pl.ds(1, REST)], psi_sem.at[1]
    )
    loads = [
        pltpu.make_async_copy(src, dst, load_sem.at[i])
        for i, (src, dst) in enumerate(
            [
                (th_hbm, th), (tl_hbm, tl), (xh_hbm, xh), (xl_hbm, xl),
                (resid_hbm, resid), (dens_hbm, dens), (din_hbm, din),
                (occ_hbm, occ),
            ]
        )
    ]
    loads[0].start()
    first_psi.start()
    loads[1].start()

    barrier = pltpu.get_barrier_semaphore()
    for n in range(KA - 1):
        pl.semaphore_signal(barrier, inc=1, device_id=(ka_peer(n), me), device_id_type=MESH)
    for peer in band_peers:
        pl.semaphore_signal(barrier, inc=1, device_id=(ka, peer), device_id_type=MESH)

    other_psi.start()
    for load in loads[2:]:
        load.start()
    loads[0].wait()
    loads[1].wait()
    first_psi.wait()

    def transform(b, store):
        columns = jnp.concatenate(
            [
                jnp.concatenate([psi_v[b, 0, p], psi_v[b, 1, p]], axis=0)
                for p in range(PLANES)
            ],
            axis=1,
        )
        along_y = times(th[...], tl[...], columns, 0)
        rows = jnp.concatenate(
            [
                jnp.concatenate(
                    [
                        along_y[:NG, p * NG : (p + 1) * NG],
                        along_y[NG:, p * NG : (p + 1) * NG],
                    ],
                    axis=1,
                )
                for p in range(PLANES)
            ],
            axis=0,
        )
        along_z = times(th[...], tl[...], rows, 1)
        for part in range(2):
            for p in range(PLANES):
                store(
                    part * PLANES + p,
                    along_z[part * NG : (part + 1) * NG, p * NG : (p + 1) * NG],
                )

    def store_a(j, block):
        send_a[pl.ds(j, NG, stride=8), :] = block

    transform(0, store_a)
    pl.semaphore_wait(barrier, NB + KA - 2)

    def start_a(n):
        peer = band_peer(n)
        pltpu.make_async_remote_copy(
            src_ref=send_a.at[pl.ds(peer * 32, 32), :],
            dst_ref=recv_a.at[me],
            send_sem=band_send.at[0],
            recv_sem=band_recv.at[0],
            device_id=(ka, peer),
            device_id_type=MESH,
        ).start()

    own_a = pltpu.make_async_copy(
        send_a.at[pl.ds(me * 32, 32), :], recv_a.at[me], own_sem.at[0]
    )

    def own_b(zi):
        return pltpu.make_async_copy(
            send_b.at[pl.ds((me * PLANES + zi) * ROWS, ROWS), :],
            recv_b.at[zi * NB + me],
            own_sem.at[zi + 1],
        )

    def start_part(zi, sem, first, count):
        rows = pl.ds(first * 8, count * 8)

        def start(n):
            peer = band_peer(n)
            pltpu.make_async_remote_copy(
                src_ref=send_b.at[
                    pl.ds((peer * PLANES + zi) * ROWS + first * 8, count * 8), :
                ],
                dst_ref=recv_b.at[zi * NB + me, rows],
                send_sem=band_send.at[sem],
                recv_sem=band_recv.at[sem],
                device_id=(ka, peer),
                device_id_type=MESH,
            ).start()

        each(NB - 1, start)

    def wait_part(zi, sems, sem, first, count):
        wait_bytes(
            recv_b.at[pl.ds(zi * NB, NB - 1), pl.ds(first * 8, count * 8)], sems.at[sem]
        )

    def start_b(zi):
        start_part(zi, zi + 1, 0, REST)
        own_b(zi).start()

    def wait_b(zi, sems):
        wait_part(zi, sems, zi + 1, 0, REST)

    def start_row(rows, sem, peer):
        pltpu.make_async_remote_copy(
            src_ref=rows.at[me],
            dst_ref=rows.at[me],
            send_sem=sem.at[0],
            recv_sem=sem.at[1],
            device_id=(ka, peer),
            device_id_type=MESH,
        ).start()

    def start_ka_row(rows, sem, peer):
        pltpu.make_async_remote_copy(
            src_ref=rows.at[ka],
            dst_ref=rows.at[ka],
            send_sem=sem.at[0],
            recv_sem=sem.at[1],
            device_id=(peer, me),
            device_id_type=MESH,
        ).start()

    def wait_rows(rows, count, sem, side):
        wait_bytes(rows.at[pl.ds(0, count - 1)], sem.at[side])

    each(NB - 1, start_a)
    own_a.start()

    def store_b(b):
        def store(j, block):
            send_b[pl.ds((b - 1) * 8 + j, NG, stride=ROWS), :] = block

        return store

    other_psi.wait()
    each(REST, lambda i: transform(i + 1, store_b(i + 1)))
    loads[7].wait()
    own_weight = jnp.full((1, 128), weights[0].astype(jnp.float32))
    w_rows[ka] = own_weight
    start_b(0)

    loads[4].wait()

    def gram_step(h):
        product = resid[h].reshape(1, PLANES * NG // 8, 8, NG) * resid[...].reshape(
            HIST, PLANES * NG // 8, 8, NG
        )
        gram_part[pl.ds(pl.multiple_of(h * HIST, HIST), HIST), :] = jnp.sum(
            jnp.sum(product, axis=1), axis=1
        )

    each(HIST, gram_step)
    each(KA - 1, lambda n: start_ka_row(w_rows, w_sem, ka_peer(n)))
    gram_rows[me] = diagonal_row(gram_part[...])

    loads[5].wait()
    loads[6].wait()
    dens[...] = dens[...] + BETA * resid[...]
    proj_part[...] = jnp.zeros((HIST, 128), jnp.float32)

    start_b(1)
    each(NB - 1, lambda n: start_row(gram_rows, gram_sem, band_peer(n)))

    wait_rows(w_rows, KA, w_sem, 1)
    factor = own_weight / jnp.sum(w_rows[...], axis=0) * jnp.float32(1.0 / NG**3)
    loads[2].wait()
    loads[3].wait()

    def operand_a(zi):
        return recv_a[:, pl.ds(pl.multiple_of(zi * 8, 8), 8), :].reshape(2 * NG, NG)

    def operand_b(zi, b):
        return recv_b[
            pl.ds(zi * NB, NB), pl.ds(pl.multiple_of((b - 1) * 8, 8), 8), :
        ].reshape(2 * NG, NG)

    def pair_power(left, right, b_left, b_right):
        field = times(xh[...], xl[...], jnp.concatenate([left, right], axis=1), 0)
        power = field[:NG] * field[:NG] + field[NG:] * field[NG:]
        return (
            power[:, :NG] * occ[0, b_left].astype(jnp.float32)
            + power[:, NG:] * occ[0, b_right].astype(jnp.float32)
        )

    def compute_plane(zi):
        plane_buf[zi] = pair_power(operand_a(zi), operand_b(zi, REST), 0, REST)

        def pair(i):
            b = 2 * i + 1
            plane_buf[zi] = plane_buf[zi] + pair_power(
                operand_b(zi, b), operand_b(zi, b + 1), b, b + 1
            )

        each(REST // 2, pair)
        plane_buf[zi] = plane_buf[zi] * factor

    def compute_last_plane(zi):
        wait_part(zi, band_recv, zi + 1, 0, REST - LATE)
        own_b(zi).wait()
        plane_buf[zi] = pair_power(operand_b(zi, 1), operand_b(zi, 2), 1, 2)

        def pair(i):
            b = 2 * i + 1
            plane_buf[zi] = plane_buf[zi] + pair_power(
                operand_b(zi, b), operand_b(zi, b + 1), b, b + 1
            )

        lax.fori_loop(1, (REST - LATE) // 2, lambda i, carry: (pair(i), carry)[1], 0)
        wait_part(zi, band_recv, zi + 2, REST - LATE, LATE)
        total = (
            plane_buf[zi]
            + pair_power(operand_b(zi, REST - 2), operand_b(zi, REST - 1), REST - 2, REST - 1)
            + pair_power(operand_a(zi), operand_b(zi, REST), 0, REST)
        )
        plane_buf[zi] = total * factor

    def start_rs(zi):
        def start(n):
            peer = x_peer(n)
            pltpu.make_async_remote_copy(
                src_ref=plane_buf.at[zi, pl.ds(peer * QUARTER, QUARTER), :],
                dst_ref=rs_buf.at[zi, x],
                send_sem=rs_send.at[zi],
                recv_sem=rs_recv.at[zi],
                device_id=(z_hi * XS + peer, me),
                device_id_type=MESH,
            ).start()

        each(XS - 1, start)

    def z_copy(zi):
        return pltpu.make_async_remote_copy(
            src_ref=z_send.at[zi],
            dst_ref=z_recv.at[zi],
            send_sem=z_ssem.at[zi],
            recv_sem=z_rsem.at[zi],
            device_id=(lax.rem(ka + XS, KA), me),
            device_id_type=MESH,
        )

    def add_up(zi):
        wait_bytes(rs_buf.at[zi, pl.ds(0, XS - 1)], rs_recv.at[zi])
        z_send[zi] = (
            plane_buf[zi, mine, :]
            + rs_buf[zi, lax.rem(x + 1, XS)]
            + rs_buf[zi, lax.rem(x + 2, XS)]
            + rs_buf[zi, lax.rem(x + 3, XS)]
        )
        z_copy(zi).start()

    def start_gather(zi):
        z_copy(zi).wait_recv()
        out_density[zi, mine, :] = z_send[zi] + z_recv[zi]

        def start(n):
            pltpu.make_async_remote_copy(
                src_ref=out_density.at[zi, mine, :],
                dst_ref=out_density.at[zi, mine, :],
                send_sem=ag_send.at[zi],
                recv_sem=ag_recv.at[zi],
                device_id=(z_hi * XS + x_peer(n), me),
                device_id_type=MESH,
            ).start()

        each(XS - 1, start)

    def project(zi):
        own = plane_buf[zi] - (1.0 / KA) * din[zi]
        product = (resid[:, zi] * own[None]).reshape(HIST, NG // 8, 8, NG)
        proj_part[...] = proj_part[...] + jnp.sum(jnp.sum(product, axis=1), axis=1)


    def invert():
        wait_rows(gram_rows, NB, gram_sem, 1)
        gram_part[...] = spread_rows(jnp.sum(gram_rows[...], axis=0), HIST * HIST)

        def entry(i, j):
            return gram_part[i * HIST + j : i * HIST + j + 1, :]

        lower, pivots = {}, []
        for j in range(HIST):
            pivot = entry(j, j) * (1.0 + REGULAR)
            for k in range(j):
                pivot = pivot - lower[j, k] * lower[j, k]
            pivots.append(1.0 / jnp.sqrt(pivot))
            for i in range(j + 1, HIST):
                value = entry(i, j)
                for k in range(j):
                    value = value - lower[i, k] * lower[j, k]
                lower[i, j] = value * pivots[j]
        unlower = {}
        for j in range(HIST):
            unlower[j, j] = pivots[j]
            for i in range(j + 1, HIST):
                value = lower[i, j] * unlower[j, j]
                for k in range(j + 1, i):
                    value = value + lower[i, k] * unlower[k, j]
                unlower[i, j] = -value * pivots[i]
        lane = lax.broadcasted_iota(jnp.int32, (1, 128), 1)
        for i in range(HIST):
            row = jnp.zeros((1, 128), jnp.float32)
            for j in range(HIST):
                value = sum(unlower[k, i] * unlower[k, j] for k in range(max(i, j), HIST))
                row = jnp.where(lane == j, value, row)
            inverse[i : i + 1, :] = row

    def early(zi):
        wait_b(zi, band_recv)
        own_b(zi).wait()
        compute_plane(zi)
        start_rs(zi)
        project(zi)
        add_up(zi)

        @pl.when(zi == 0)
        def _():
            start_b(2)

        @pl.when(zi == 1)
        def _():
            start_part(last, last + 1, 0, REST - LATE)
            own_b(last).start()
            start_part(last, last + 2, REST - LATE, LATE)

        @pl.when(zi > 0)
        def _():
            start_gather(zi - 1)

        @pl.when(zi == 1)
        def _():
            invert()

    wait_bytes(recv_a.at[pl.ds(0, NB - 1)], band_recv.at[0])
    own_a.wait()
    each(last, early)

    wait_bytes(recv_a.at[pl.ds(0, NB - 1)], band_send.at[0])
    for zi in range(PLANES - 2):
        wait_b(zi, band_send)
    wait_rows(w_rows, KA, w_sem, 0)
    wait_rows(gram_rows, NB, gram_sem, 0)

    compute_last_plane(last)
    start_rs(last)
    project(last)
    proj_rows[me] = diagonal_row(proj_part[...])
    for peer in band_peers:
        start_row(proj_rows, proj_sem, peer)
    add_up(last)
    start_gather(last - 1)
    wait_rows(proj_rows, NB, proj_sem, 1)
    total_rows[ka] = jnp.sum(proj_rows[...], axis=0)
    each(KA - 1, lambda n: start_ka_row(total_rows, total_sem, ka_peer(n)))
    start_gather(last)

    wait_b(last - 1, band_send)
    wait_part(last, band_send, last + 1, 0, REST - LATE)
    wait_part(last, band_send, last + 2, REST - LATE, LATE)
    wait_rows(proj_rows, NB, proj_sem, 0)
    for zi in range(PLANES):
        wait_bytes(rs_buf.at[zi, pl.ds(0, XS - 1)], rs_send.at[zi])
        z_copy(zi).wait_send()

    wait_rows(total_rows, KA, total_sem, 1)
    projections = jnp.sum(total_rows[...], axis=0)
    coefs = jnp.sum(inverse[...] * projections, axis=1, keepdims=True)
    for zi in range(PLANES):
        wait_bytes(out_density.at[zi, pl.ds(0, NG - QUARTER), :], ag_recv.at[zi])
        update = coefs[0:1] * dens[0, zi]
        for h in range(1, HIST):
            update = update + coefs[h : h + 1] * dens[h, zi]
        out_mixed[zi] = din[zi] + BETA * (out_density[zi] - din[zi]) - update

    wait_rows(total_rows, KA, total_sem, 0)
    for zi in range(PLANES):
        wait_bytes(out_density.at[zi, pl.ds(0, NG - QUARTER), :], ag_send.at[zi])


def write_out(density, mixed, out_density, out_mixed, sems):
    copies = [
        pltpu.make_async_copy(density, out_density, sems.at[0]),
        pltpu.make_async_copy(mixed, out_mixed, sems.at[1]),
    ]
    for copy in copies:
        copy.start()
    for copy in copies:
        copy.wait()


def shards(psi_hat, occupations, weights, density_in, dens_hist, resid_hist):
    operands = (occupations, psi_hat, density_in, dens_hist, resid_hist)
    operands += tuple(jnp.asarray(table) for table in dft_tables())
    plane = (PLANES, NG, NG)
    f32 = jnp.float32
    dma = pltpu.SemaphoreType.DMA
    vmem = partial(pltpu.VMEM)
    hbm_spec = pl.BlockSpec(memory_space=pltpu.HBM)
    vmem_spec = pl.BlockSpec(memory_space=pltpu.VMEM)
    table = vmem((2 * NG, 2 * NG), jnp.bfloat16)
    density, mixed = pl.pallas_call(
        kernel,
        out_shape=(jax.ShapeDtypeStruct(plane, f32), jax.ShapeDtypeStruct(plane, f32)),
        in_specs=[pl.BlockSpec(memory_space=pltpu.SMEM)] + [hbm_spec] * 9,
        out_specs=(vmem_spec, vmem_spec),
        scratch_shapes=[
            pltpu.SMEM((1, BANDS), jnp.int32),
            vmem((BANDS, 2, PLANES, NG, NG), f32),
            vmem(plane, f32),
            vmem((HIST, *plane), f32),
            vmem((HIST, *plane), f32),
            table, table, table, table,
            vmem((NG * 8, NG), f32),
            vmem((NG * ROWS, NG), f32),
            vmem((NB, 8 * PLANES, NG), f32),
            vmem((PLANES * NB, ROWS, NG), f32),
            vmem(plane, f32),
            vmem((PLANES, XS, QUARTER, NG), f32),
            vmem((PLANES, QUARTER, NG), f32),
            vmem((PLANES, QUARTER, NG), f32),
            vmem((HIST * HIST, 128), f32),
            vmem((NB, 1, 128), f32),
            vmem((HIST, 128), f32),
            vmem((NB, 1, 128), f32),
            vmem((KA, 1, 128), f32),
            vmem((KA, 1, 128), f32),
            vmem((HIST, 128), f32),
            dma((2,)), dma((8,)), dma((CHUNKS,)),
            dma((CHUNKS,)), dma((CHUNKS,)),
            dma((PLANES,)), dma((PLANES,)),
            dma((PLANES,)), dma((PLANES,)),
            dma((PLANES,)), dma((PLANES,)),
            dma((2,)), dma((2,)), dma((2,)), dma((2,)),
        ],
        compiler_params=pltpu.CompilerParams(
            collective_id=0, has_side_effects=True, vmem_limit_bytes=32 * 1024 * 1024
        ),
    )(weights, *(pltpu.with_memory_space_constraint(operand, pltpu.HBM) for operand in operands))
    return pl.pallas_call(
        write_out,
        out_shape=(jax.ShapeDtypeStruct(plane, f32), jax.ShapeDtypeStruct(plane, f32)),
        in_specs=[vmem_spec, vmem_spec],
        out_specs=(hbm_spec, hbm_spec),
        scratch_shapes=[dma((2,))],
        compiler_params=pltpu.CompilerParams(vmem_limit_bytes=1024 * 1024),
    )(density, mixed)


def solution(mesh):
    return jax.shard_map(
        shards,
        mesh=mesh,
        in_specs=(
            P("ka", None, None, "band", None, None),
            P("ka", None),
            P("ka"),
            P("band", None, None),
            P(None, "band", None, None),
            P(None, "band", None, None),
        ),
        out_specs=(P("band", None, None), P("band", None, None)),
        check_vma=False,
    )
```

```python
from functools import partial

import jax
import jax.numpy as jnp
import ml_dtypes
import numpy as np
from jax import lax
from jax.experimental import pallas as pl
from jax.experimental.pallas import tpu as pltpu
from jax.sharding import PartitionSpec as P

NG = 128
BANDS = 12
HIST = 8
KA = 8
NB = 32
XS = 4
PLANES = NG // NB
REST = BANDS - 1
ROWS = REST * 8
QUARTER = NG // XS
LATE = 3
CHUNKS = PLANES + 2
BETA = 0.3
REGULAR = 0.01
MESH = pl.DeviceIdType.MESH


def split_table(table):
    high = table.astype(ml_dtypes.bfloat16)
    low = (table - high.astype(np.float64)).astype(ml_dtypes.bfloat16)
    return high, low


def dft_tables():
    index = np.arange(NG)
    angles = 2.0 * np.pi * (index[:, None] * index[None, :] % NG) / NG
    cosine, sine = np.cos(angles), np.sin(angles)
    table = np.block([[cosine, -sine], [sine, cosine]])
    order = [
        part * NG + source * PLANES + p
        for source in range(NB)
        for part in range(2)
        for p in range(PLANES)
    ]
    return (*split_table(table), *split_table(table[:, order]))


def split(x):
    high = x.astype(jnp.bfloat16)
    low = (x - high.astype(jnp.float32)).astype(jnp.bfloat16)
    return high, low


def times(table_high, table_low, x, contract):
    high, low = split(x)
    dot = partial(
        lax.dot_general,
        dimension_numbers=(((1,), (contract,)), ((), ())),
        preferred_element_type=jnp.float32,
    )
    return dot(table_high, high) + (dot(table_low, high) + dot(table_high, low))


def diagonal_row(columns):
    sums = jnp.sum(columns, axis=1, keepdims=True)
    shape = columns.shape
    on = lax.broadcasted_iota(jnp.int32, shape, 0) == lax.broadcasted_iota(jnp.int32, shape, 1)
    return jnp.sum(jnp.where(on, sums, 0.0), axis=0, keepdims=True)


def spread_rows(row, count):
    shape = (count, 128)
    on = lax.broadcasted_iota(jnp.int32, shape, 0) == lax.broadcasted_iota(jnp.int32, shape, 1)
    picked = jnp.sum(jnp.where(on, row, 0.0), axis=1, keepdims=True)
    return jnp.broadcast_to(picked, shape)


def kernel(
    weights, occ_hbm, psi, din_hbm, dens_hbm, resid_hbm, th_hbm, tl_hbm, xh_hbm, xl_hbm,
    out_density, out_mixed,
    occ, psi_v, din, dens, resid, th, tl, xh, xl,
    send_a, send_b, recv_a, recv_b,
    plane_buf, rs_buf, z_send, z_recv, gram_part, gram_rows, proj_part, proj_rows, total_rows, w_rows, inverse,
    psi_sem, load_sem, own_sem,
    band_send, band_recv, rs_send, rs_recv, z_ssem, z_rsem, ag_send, ag_recv,
    gram_sem, proj_sem, total_sem, w_sem,
):
    ka = lax.axis_index("ka")
    me = lax.axis_index("band")
    z_hi, x = lax.div(ka, XS), lax.rem(ka, XS)
    y, z, core = lax.div(me, 8), lax.rem(lax.div(me, 2), 4), lax.rem(me, 2)

    half = lax.div(z, 2)
    z_end, z_middle, z_beside = 3 - 3 * half, 2 - half, half * 2 + 1 - lax.rem(z, 2)

    def band_peer(n):
        i, dy = lax.div(n, 4), 3 - lax.rem(n, 4)
        z_far = jnp.where(lax.rem(i, 2) == 0, z_end, z_middle)
        z_near = jnp.where(i < 6, z_beside, z)
        core_near = jnp.where(i < 6, i - 4, jnp.where(i == 6, 1 - core, core))
        z_to = jnp.where(i < 4, z_far, z_near)
        core_to = jnp.where(i < 4, lax.div(i, 2), core_near)
        return lax.rem(y + dy, 4) * 8 + z_to * 2 + core_to

    y_part = [lax.rem(y + dy, 4) * 8 for dy in range(4)]
    core_part = [core, 1 - core]
    others_along_z = [z_end, z_middle, z_beside]

    def across(dx, dy, dc):
        return z_hi * XS + lax.rem(x + dx, XS), y_part[dy] + z * 2 + core_part[dc]

    flat = [(dx, dy, dc) for dx in range(XS) for dy in range(4) for dc in range(2)][1:]
    flat_peers = [across(*step) for step in flat]
    flat_slot = x * 8 + y * 2 + core
    z_slot = z_hi * 4 + z

    def along_z(dz):
        to = lax.rem(z_slot + dz, 8)
        return lax.div(to, 4) * XS + x, y * 8 + lax.rem(to, 4) * 2 + core

    z_peers = [along_z(dz) for dz in range(1, 8)]

    def ka_peer(n):
        return lax.rem(ka + 1 + n, KA)

    def x_peer(n):
        return lax.rem(x + 1 + n, XS)

    def each(count, body):
        def step(n, carry):
            body(n)
            return carry

        lax.fori_loop(0, count, step, 0)

    def wait_bytes(ref, sem):
        pltpu.make_async_copy(ref, ref, sem).wait()

    last = PLANES - 1
    mine = pl.ds(pl.multiple_of(x * QUARTER, QUARTER), QUARTER)

    first_psi = pltpu.make_async_copy(psi.at[0, 0], psi_v.at[0], psi_sem.at[0])
    other_psi = pltpu.make_async_copy(
        psi.at[0, pl.ds(1, REST)], psi_v.at[pl.ds(1, REST)], psi_sem.at[1]
    )
    loads = [
        pltpu.make_async_copy(src, dst, load_sem.at[i])
        for i, (src, dst) in enumerate(
            [
                (th_hbm, th), (tl_hbm, tl), (xh_hbm, xh), (xl_hbm, xl),
                (resid_hbm, resid), (dens_hbm, dens), (din_hbm, din),
                (occ_hbm, occ),
            ]
        )
    ]
    loads[0].start()
    first_psi.start()
    loads[1].start()

    barrier = pltpu.get_barrier_semaphore()
    for device in z_peers + flat_peers:
        pl.semaphore_signal(barrier, inc=1, device_id=device, device_id_type=MESH)
    other_half = XS - z_hi * XS
    for dx in range(1, XS):
        device = (other_half + lax.rem(x + dx, XS), me)
        pl.semaphore_signal(barrier, inc=1, device_id=device, device_id_type=MESH)
    for z_to in others_along_z:
        for dy, dc in [(dy, dc) for dy in range(4) for dc in range(2)][1:]:
            device = (ka, y_part[dy] + z_to * 2 + core_part[dc])
            pl.semaphore_signal(barrier, inc=1, device_id=device, device_id_type=MESH)

    other_psi.start()
    for load in loads[2:]:
        load.start()
    loads[0].wait()
    loads[1].wait()
    first_psi.wait()

    def transform(b, store):
        columns = jnp.concatenate(
            [
                jnp.concatenate([psi_v[b, 0, p], psi_v[b, 1, p]], axis=0)
                for p in range(PLANES)
            ],
            axis=1,
        )
        along_y = times(th[...], tl[...], columns, 0)
        rows = jnp.concatenate(
            [
                jnp.concatenate(
                    [
                        along_y[:NG, p * NG : (p + 1) * NG],
                        along_y[NG:, p * NG : (p + 1) * NG],
                    ],
                    axis=1,
                )
                for p in range(PLANES)
            ],
            axis=0,
        )
        along_z = times(th[...], tl[...], rows, 1)
        for part in range(2):
            for p in range(PLANES):
                store(
                    part * PLANES + p,
                    along_z[part * NG : (part + 1) * NG, p * NG : (p + 1) * NG],
                )

    def store_a(j, block):
        send_a[pl.ds(j, NG, stride=8), :] = block

    transform(0, store_a)
    pl.semaphore_wait(barrier, 7 + NB - 1 + XS - 1 + 21)

    def start_a(n):
        peer = band_peer(n)
        pltpu.make_async_remote_copy(
            src_ref=send_a.at[pl.ds(peer * 32, 32), :],
            dst_ref=recv_a.at[me],
            send_sem=band_send.at[0],
            recv_sem=band_recv.at[0],
            device_id=(ka, peer),
            device_id_type=MESH,
        ).start()

    own_a = pltpu.make_async_copy(
        send_a.at[pl.ds(me * 32, 32), :], recv_a.at[me], own_sem.at[0]
    )

    def own_b(zi):
        return pltpu.make_async_copy(
            send_b.at[pl.ds((me * PLANES + zi) * ROWS, ROWS), :],
            recv_b.at[zi * NB + me],
            own_sem.at[zi + 1],
        )

    def start_part(zi, sem, first, count):
        rows = pl.ds(first * 8, count * 8)

        def start(n):
            peer = band_peer(n)
            pltpu.make_async_remote_copy(
                src_ref=send_b.at[
                    pl.ds((peer * PLANES + zi) * ROWS + first * 8, count * 8), :
                ],
                dst_ref=recv_b.at[zi * NB + me, rows],
                send_sem=band_send.at[sem],
                recv_sem=band_recv.at[sem],
                device_id=(ka, peer),
                device_id_type=MESH,
            ).start()

        each(NB - 1, start)

    def wait_part(zi, sems, sem, first, count):
        wait_bytes(
            recv_b.at[pl.ds(zi * NB, NB - 1), pl.ds(first * 8, count * 8)], sems.at[sem]
        )

    def start_b(zi):
        start_part(zi, zi + 1, 0, REST)
        own_b(zi).start()

    def wait_b(zi, sems):
        wait_part(zi, sems, zi + 1, 0, REST)

    def start_slot(rows, slot, sem, device):
        pltpu.make_async_remote_copy(
            src_ref=rows.at[slot],
            dst_ref=rows.at[slot],
            send_sem=sem.at[0],
            recv_sem=sem.at[1],
            device_id=device,
            device_id_type=MESH,
        ).start()

    def wait_rows(rows, count, sem, side):
        wait_bytes(rows.at[pl.ds(0, count - 1)], sem.at[side])

    each(NB - 1, start_a)
    own_a.start()

    def store_b(b):
        def store(j, block):
            send_b[pl.ds((b - 1) * 8 + j, NG, stride=ROWS), :] = block

        return store

    other_psi.wait()
    each(REST, lambda i: transform(i + 1, store_b(i + 1)))
    loads[7].wait()
    own_weight = jnp.full((1, 128), weights[0].astype(jnp.float32))
    w_rows[ka] = own_weight
    start_b(0)

    loads[4].wait()

    def gram_step(h):
        product = resid[h].reshape(1, PLANES * NG // 8, 8, NG) * resid[...].reshape(
            HIST, PLANES * NG // 8, 8, NG
        )
        gram_part[pl.ds(pl.multiple_of(h * HIST, HIST), HIST), :] = jnp.sum(
            jnp.sum(product, axis=1), axis=1
        )

    each(HIST, gram_step)
    each(KA - 1, lambda n: start_slot(w_rows, ka, w_sem, (ka_peer(n), me)))
    gram_rows[me] = diagonal_row(gram_part[...])

    loads[5].wait()
    loads[6].wait()
    dens[...] = dens[...] + BETA * resid[...]
    proj_part[...] = jnp.zeros((HIST, 128), jnp.float32)

    start_b(1)
    each(NB - 1, lambda n: start_slot(gram_rows, me, gram_sem, (ka, band_peer(n))))

    wait_rows(w_rows, KA, w_sem, 1)
    factor = own_weight / jnp.sum(w_rows[...], axis=0) * jnp.float32(1.0 / NG**3)
    loads[2].wait()
    loads[3].wait()

    def operand_a(zi):
        return recv_a[:, pl.ds(pl.multiple_of(zi * 8, 8), 8), :].reshape(2 * NG, NG)

    def operand_b(zi, b):
        return recv_b[
            pl.ds(zi * NB, NB), pl.ds(pl.multiple_of((b - 1) * 8, 8), 8), :
        ].reshape(2 * NG, NG)

    def pair_power(left, right, b_left, b_right):
        field = times(xh[...], xl[...], jnp.concatenate([left, right], axis=1), 0)
        power = field[:NG] * field[:NG] + field[NG:] * field[NG:]
        return (
            power[:, :NG] * occ[0, b_left].astype(jnp.float32)
            + power[:, NG:] * occ[0, b_right].astype(jnp.float32)
        )

    def compute_plane(zi):
        plane_buf[zi] = pair_power(operand_a(zi), operand_b(zi, REST), 0, REST)

        def pair(i):
            b = 2 * i + 1
            plane_buf[zi] = plane_buf[zi] + pair_power(
                operand_b(zi, b), operand_b(zi, b + 1), b, b + 1
            )

        each(REST // 2, pair)
        plane_buf[zi] = plane_buf[zi] * factor

    def compute_last_plane(zi):
        wait_part(zi, band_recv, zi + 1, 0, REST - LATE)
        own_b(zi).wait()
        plane_buf[zi] = pair_power(operand_b(zi, 1), operand_b(zi, 2), 1, 2)

        def pair(i):
            b = 2 * i + 1
            plane_buf[zi] = plane_buf[zi] + pair_power(
                operand_b(zi, b), operand_b(zi, b + 1), b, b + 1
            )

        lax.fori_loop(1, (REST - LATE) // 2, lambda i, carry: (pair(i), carry)[1], 0)
        wait_part(zi, band_recv, zi + 2, REST - LATE, LATE)
        total = (
            plane_buf[zi]
            + pair_power(operand_b(zi, REST - 2), operand_b(zi, REST - 1), REST - 2, REST - 1)
            + pair_power(operand_a(zi), operand_b(zi, REST), 0, REST)
        )
        plane_buf[zi] = total * factor

    def start_rs(zi):
        def start(n):
            peer = x_peer(n)
            pltpu.make_async_remote_copy(
                src_ref=plane_buf.at[zi, pl.ds(peer * QUARTER, QUARTER), :],
                dst_ref=rs_buf.at[zi, x],
                send_sem=rs_send.at[zi],
                recv_sem=rs_recv.at[zi],
                device_id=(z_hi * XS + peer, me),
                device_id_type=MESH,
            ).start()

        each(XS - 1, start)

    def z_copy(zi):
        return pltpu.make_async_remote_copy(
            src_ref=z_send.at[zi],
            dst_ref=z_recv.at[zi],
            send_sem=z_ssem.at[zi],
            recv_sem=z_rsem.at[zi],
            device_id=(lax.rem(ka + XS, KA), me),
            device_id_type=MESH,
        )

    def add_up(zi):
        wait_bytes(rs_buf.at[zi, pl.ds(0, XS - 1)], rs_recv.at[zi])
        z_send[zi] = (
            plane_buf[zi, mine, :]
            + rs_buf[zi, lax.rem(x + 1, XS)]
            + rs_buf[zi, lax.rem(x + 2, XS)]
            + rs_buf[zi, lax.rem(x + 3, XS)]
        )
        z_copy(zi).start()

    def start_gather(zi):
        z_copy(zi).wait_recv()
        out_density[zi, mine, :] = z_send[zi] + z_recv[zi]

        def start(n):
            pltpu.make_async_remote_copy(
                src_ref=out_density.at[zi, mine, :],
                dst_ref=out_density.at[zi, mine, :],
                send_sem=ag_send.at[zi],
                recv_sem=ag_recv.at[zi],
                device_id=(z_hi * XS + x_peer(n), me),
                device_id_type=MESH,
            ).start()

        each(XS - 1, start)

    def project(zi):
        own = plane_buf[zi] - (1.0 / KA) * din[zi]
        product = (resid[:, zi] * own[None]).reshape(HIST, NG // 8, 8, NG)
        proj_part[...] = proj_part[...] + jnp.sum(jnp.sum(product, axis=1), axis=1)


    def invert():
        wait_rows(gram_rows, NB, gram_sem, 1)
        gram_part[...] = spread_rows(jnp.sum(gram_rows[...], axis=0), HIST * HIST)

        def entry(i, j):
            return gram_part[i * HIST + j : i * HIST + j + 1, :]

        lower, pivots = {}, []
        for j in range(HIST):
            pivot = entry(j, j) * (1.0 + REGULAR)
            for k in range(j):
                pivot = pivot - lower[j, k] * lower[j, k]
            pivots.append(1.0 / jnp.sqrt(pivot))
            for i in range(j + 1, HIST):
                value = entry(i, j)
                for k in range(j):
                    value = value - lower[i, k] * lower[j, k]
                lower[i, j] = value * pivots[j]
        unlower = {}
        for j in range(HIST):
            unlower[j, j] = pivots[j]
            for i in range(j + 1, HIST):
                value = lower[i, j] * unlower[j, j]
                for k in range(j + 1, i):
                    value = value + lower[i, k] * unlower[k, j]
                unlower[i, j] = -value * pivots[i]
        lane = lax.broadcasted_iota(jnp.int32, (1, 128), 1)
        for i in range(HIST):
            row = jnp.zeros((1, 128), jnp.float32)
            for j in range(HIST):
                value = sum(unlower[k, i] * unlower[k, j] for k in range(max(i, j), HIST))
                row = jnp.where(lane == j, value, row)
            inverse[i : i + 1, :] = row

    def early(zi):
        wait_b(zi, band_recv)
        own_b(zi).wait()
        compute_plane(zi)
        start_rs(zi)
        project(zi)
        add_up(zi)

        @pl.when(zi == 0)
        def _():
            start_b(2)

        @pl.when(zi == 1)
        def _():
            start_part(last, last + 1, 0, REST - LATE)
            own_b(last).start()
            start_part(last, last + 2, REST - LATE, LATE)

        @pl.when(zi > 0)
        def _():
            start_gather(zi - 1)

        @pl.when(zi == 1)
        def _():
            invert()

    wait_bytes(recv_a.at[pl.ds(0, NB - 1)], band_recv.at[0])
    own_a.wait()
    each(last, early)

    wait_bytes(recv_a.at[pl.ds(0, NB - 1)], band_send.at[0])
    for zi in range(PLANES - 2):
        wait_b(zi, band_send)
    wait_rows(w_rows, KA, w_sem, 0)
    wait_rows(gram_rows, NB, gram_sem, 0)

    compute_last_plane(last)
    start_rs(last)
    project(last)
    proj_rows[flat_slot] = diagonal_row(proj_part[...])
    for device in flat_peers:
        start_slot(proj_rows, flat_slot, proj_sem, device)
    add_up(last)
    start_gather(last - 1)
    wait_rows(proj_rows, NB, proj_sem, 1)
    total_rows[z_slot] = jnp.sum(proj_rows[...], axis=0)
    for device in z_peers:
        start_slot(total_rows, z_slot, total_sem, device)
    start_gather(last)

    wait_b(last - 1, band_send)
    wait_part(last, band_send, last + 1, 0, REST - LATE)
    wait_part(last, band_send, last + 2, REST - LATE, LATE)
    wait_rows(proj_rows, NB, proj_sem, 0)
    for zi in range(PLANES):
        wait_bytes(rs_buf.at[zi, pl.ds(0, XS - 1)], rs_send.at[zi])
        z_copy(zi).wait_send()

    wait_rows(total_rows, KA, total_sem, 1)
    projections = jnp.sum(total_rows[...], axis=0)
    coefs = jnp.sum(inverse[...] * projections, axis=1, keepdims=True)
    for zi in range(PLANES):
        wait_bytes(out_density.at[zi, pl.ds(0, NG - QUARTER), :], ag_recv.at[zi])
        update = coefs[0:1] * dens[0, zi]
        for h in range(1, HIST):
            update = update + coefs[h : h + 1] * dens[h, zi]
        out_mixed[zi] = din[zi] + BETA * (out_density[zi] - din[zi]) - update

    wait_rows(total_rows, KA, total_sem, 0)
    for zi in range(PLANES):
        wait_bytes(out_density.at[zi, pl.ds(0, NG - QUARTER), :], ag_send.at[zi])


def write_out(density, mixed, out_density, out_mixed, sems):
    copies = [
        pltpu.make_async_copy(density, out_density, sems.at[0]),
        pltpu.make_async_copy(mixed, out_mixed, sems.at[1]),
    ]
    for copy in copies:
        copy.start()
    for copy in copies:
        copy.wait()


def shards(psi_hat, occupations, weights, density_in, dens_hist, resid_hist):
    operands = (occupations, psi_hat, density_in, dens_hist, resid_hist)
    operands += tuple(jnp.asarray(table) for table in dft_tables())
    plane = (PLANES, NG, NG)
    f32 = jnp.float32
    dma = pltpu.SemaphoreType.DMA
    vmem = partial(pltpu.VMEM)
    hbm_spec = pl.BlockSpec(memory_space=pltpu.HBM)
    vmem_spec = pl.BlockSpec(memory_space=pltpu.VMEM)
    table = vmem((2 * NG, 2 * NG), jnp.bfloat16)
    density, mixed = pl.pallas_call(
        kernel,
        out_shape=(jax.ShapeDtypeStruct(plane, f32), jax.ShapeDtypeStruct(plane, f32)),
        in_specs=[pl.BlockSpec(memory_space=pltpu.SMEM)] + [hbm_spec] * 9,
        out_specs=(vmem_spec, vmem_spec),
        scratch_shapes=[
            pltpu.SMEM((1, BANDS), jnp.int32),
            vmem((BANDS, 2, PLANES, NG, NG), f32),
            vmem(plane, f32),
            vmem((HIST, *plane), f32),
            vmem((HIST, *plane), f32),
            table, table, table, table,
            vmem((NG * 8, NG), f32),
            vmem((NG * ROWS, NG), f32),
            vmem((NB, 8 * PLANES, NG), f32),
            vmem((PLANES * NB, ROWS, NG), f32),
            vmem(plane, f32),
            vmem((PLANES, XS, QUARTER, NG), f32),
            vmem((PLANES, QUARTER, NG), f32),
            vmem((PLANES, QUARTER, NG), f32),
            vmem((HIST * HIST, 128), f32),
            vmem((NB, 1, 128), f32),
            vmem((HIST, 128), f32),
            vmem((NB, 1, 128), f32),
            vmem((KA, 1, 128), f32),
            vmem((KA, 1, 128), f32),
            vmem((HIST, 128), f32),
            dma((2,)), dma((8,)), dma((CHUNKS,)),
            dma((CHUNKS,)), dma((CHUNKS,)),
            dma((PLANES,)), dma((PLANES,)),
            dma((PLANES,)), dma((PLANES,)),
            dma((PLANES,)), dma((PLANES,)),
            dma((2,)), dma((2,)), dma((2,)), dma((2,)),
        ],
        compiler_params=pltpu.CompilerParams(
            collective_id=0, has_side_effects=True, vmem_limit_bytes=32 * 1024 * 1024
        ),
    )(weights, *(pltpu.with_memory_space_constraint(operand, pltpu.HBM) for operand in operands))
    return pl.pallas_call(
        write_out,
        out_shape=(jax.ShapeDtypeStruct(plane, f32), jax.ShapeDtypeStruct(plane, f32)),
        in_specs=[vmem_spec, vmem_spec],
        out_specs=(hbm_spec, hbm_spec),
        scratch_shapes=[dma((2,))],
        compiler_params=pltpu.CompilerParams(vmem_limit_bytes=1024 * 1024),
    )(density, mixed)


def solution(mesh):
    return jax.shard_map(
        shards,
        mesh=mesh,
        in_specs=(
            P("ka", None, None, "band", None, None),
            P("ka", None),
            P("ka"),
            P("band", None, None),
            P(None, "band", None, None),
            P(None, "band", None, None),
        ),
        out_specs=(P("band", None, None), P("band", None, None)),
        check_vma=False,
    )
```

```python
from functools import partial

import jax
import jax.numpy as jnp
import ml_dtypes
import numpy as np
from jax import lax
from jax.experimental import pallas as pl
from jax.experimental.pallas import tpu as pltpu
from jax.sharding import PartitionSpec as P

NG = 128
BANDS = 12
HIST = 8
KA = 8
NB = 32
XS = 4
PLANES = NG // NB
REST = BANDS - 1
ROWS = REST * 8
QUARTER = NG // XS
LATE = 3
CHUNKS = PLANES + 2
BETA = 0.3
REGULAR = 0.01
MESH = pl.DeviceIdType.MESH


def split_table(table):
    high = table.astype(ml_dtypes.bfloat16)
    low = (table - high.astype(np.float64)).astype(ml_dtypes.bfloat16)
    return high, low


def dft_tables():
    index = np.arange(NG)
    angles = 2.0 * np.pi * (index[:, None] * index[None, :] % NG) / NG
    cosine, sine = np.cos(angles), np.sin(angles)
    table = np.block([[cosine, -sine], [sine, cosine]])
    order = [
        part * NG + source * PLANES + p
        for source in range(NB)
        for part in range(2)
        for p in range(PLANES)
    ]
    return (*split_table(table), *split_table(table[:, order]))


def split(x):
    high = x.astype(jnp.bfloat16)
    low = (x - high.astype(jnp.float32)).astype(jnp.bfloat16)
    return high, low


def times(table_high, table_low, x, contract):
    high, low = split(x)
    dot = partial(
        lax.dot_general,
        dimension_numbers=(((1,), (contract,)), ((), ())),
        preferred_element_type=jnp.float32,
    )
    return dot(table_high, high) + (dot(table_low, high) + dot(table_high, low))


def diagonal_row(columns):
    sums = jnp.sum(columns, axis=1, keepdims=True)
    shape = columns.shape
    on = lax.broadcasted_iota(jnp.int32, shape, 0) == lax.broadcasted_iota(jnp.int32, shape, 1)
    return jnp.sum(jnp.where(on, sums, 0.0), axis=0, keepdims=True)


def spread_rows(row, count):
    shape = (count, 128)
    on = lax.broadcasted_iota(jnp.int32, shape, 0) == lax.broadcasted_iota(jnp.int32, shape, 1)
    picked = jnp.sum(jnp.where(on, row, 0.0), axis=1, keepdims=True)
    return jnp.broadcast_to(picked, shape)


def kernel(
    weights, occ_hbm, psi, din_hbm, dens_hbm, resid_hbm, th_hbm, tl_hbm, xh_hbm, xl_hbm,
    out_density, out_mixed,
    occ, psi_v, din, dens, resid, th, tl, xh, xl,
    send_a, send_b, recv_a, recv_b,
    plane_buf, rs_buf, z_send, z_recv, gram_part, gram_rows, proj_part, proj_rows, total_rows, w_rows, inverse,
    psi_sem, load_sem, own_sem,
    band_send, band_recv, rs_send, rs_recv, z_ssem, z_rsem, ag_send, ag_recv,
    gram_sem, proj_sem, total_sem, w_sem,
):
    ka = lax.axis_index("ka")
    me = lax.axis_index("band")
    z_hi, x = lax.div(ka, XS), lax.rem(ka, XS)
    y, z, core = lax.div(me, 8), lax.rem(lax.div(me, 2), 4), lax.rem(me, 2)

    half = lax.div(z, 2)
    z_end, z_middle, z_beside = 3 - 3 * half, 2 - half, half * 2 + 1 - lax.rem(z, 2)

    def band_peer(n):
        i, dy = lax.div(n, 4), 3 - lax.rem(n, 4)
        z_far = jnp.where(lax.rem(i, 2) == 0, z_end, z_middle)
        z_near = jnp.where(i < 6, z_beside, z)
        core_near = jnp.where(i < 6, i - 4, jnp.where(i == 6, 1 - core, core))
        z_to = jnp.where(i < 4, z_far, z_near)
        core_to = jnp.where(i < 4, lax.div(i, 2), core_near)
        return lax.rem(y + dy, 4) * 8 + z_to * 2 + core_to

    y_part = [lax.rem(y + dy, 4) * 8 for dy in range(4)]
    core_part = [core, 1 - core]
    others_along_z = [z_end, z_middle, z_beside]

    def across(dx, dy, dc):
        return z_hi * XS + lax.rem(x + dx, XS), y_part[dy] + z * 2 + core_part[dc]

    flat = [(dx, dy, dc) for dx in range(XS) for dy in range(4) for dc in range(2)][1:]
    flat_peers = [across(*step) for step in flat]
    flat_slot = x * 8 + y * 2 + core
    z_slot = z_hi * 4 + z

    def along_z(dz):
        to = lax.rem(z_slot + dz, 8)
        return lax.div(to, 4) * XS + x, y * 8 + lax.rem(to, 4) * 2 + core

    z_peers = [along_z(dz) for dz in range(1, 8)]

    def ka_peer(n):
        return lax.rem(ka + 1 + n, KA)

    def x_peer(n):
        return lax.rem(x + 1 + n, XS)

    def each(count, body):
        def step(n, carry):
            body(n)
            return carry

        lax.fori_loop(0, count, step, 0)

    def wait_bytes(ref, sem):
        pltpu.make_async_copy(ref, ref, sem).wait()

    last = PLANES - 1
    mine = pl.ds(pl.multiple_of(x * QUARTER, QUARTER), QUARTER)

    first_psi = pltpu.make_async_copy(psi.at[0, 0], psi_v.at[0], psi_sem.at[0])
    other_psi = pltpu.make_async_copy(
        psi.at[0, pl.ds(1, REST)], psi_v.at[pl.ds(1, REST)], psi_sem.at[1]
    )
    loads = [
        pltpu.make_async_copy(src, dst, load_sem.at[i])
        for i, (src, dst) in enumerate(
            [
                (th_hbm, th), (tl_hbm, tl), (xh_hbm, xh), (xl_hbm, xl),
                (resid_hbm, resid), (dens_hbm, dens), (din_hbm, din),
                (occ_hbm, occ),
            ]
        )
    ]
    loads[0].start()
    first_psi.start()
    loads[1].start()

    barrier = pltpu.get_barrier_semaphore()
    for device in z_peers + flat_peers:
        pl.semaphore_signal(barrier, inc=1, device_id=device, device_id_type=MESH)
    other_half = XS - z_hi * XS
    for dx in range(1, XS):
        device = (other_half + lax.rem(x + dx, XS), me)
        pl.semaphore_signal(barrier, inc=1, device_id=device, device_id_type=MESH)
    for z_to in others_along_z:
        for dy, dc in [(dy, dc) for dy in range(4) for dc in range(2)][1:]:
            device = (ka, y_part[dy] + z_to * 2 + core_part[dc])
            pl.semaphore_signal(barrier, inc=1, device_id=device, device_id_type=MESH)

    other_psi.start()
    for load in loads[2:]:
        load.start()
    loads[0].wait()
    loads[1].wait()
    first_psi.wait()

    def transform(b, store):
        columns = jnp.concatenate(
            [
                jnp.concatenate([psi_v[b, 0, p], psi_v[b, 1, p]], axis=0)
                for p in range(PLANES)
            ],
            axis=1,
        )
        along_y = times(th[...], tl[...], columns, 0)
        rows = jnp.concatenate(
            [
                jnp.concatenate(
                    [
                        along_y[:NG, p * NG : (p + 1) * NG],
                        along_y[NG:, p * NG : (p + 1) * NG],
                    ],
                    axis=1,
                )
                for p in range(PLANES)
            ],
            axis=0,
        )
        along_z = times(th[...], tl[...], rows, 1)
        for part in range(2):
            for p in range(PLANES):
                store(
                    part * PLANES + p,
                    along_z[part * NG : (part + 1) * NG, p * NG : (p + 1) * NG],
                )

    def store_a(j, block):
        send_a[pl.ds(j, NG, stride=8), :] = block

    transform(0, store_a)
    pl.semaphore_wait(barrier, 7 + NB - 1 + XS - 1 + 21)

    def start_a(n):
        peer = band_peer(n)
        pltpu.make_async_remote_copy(
            src_ref=send_a.at[pl.ds(peer * 32, 32), :],
            dst_ref=recv_a.at[me],
            send_sem=band_send.at[0],
            recv_sem=band_recv.at[0],
            device_id=(ka, peer),
            device_id_type=MESH,
        ).start()

    own_a = pltpu.make_async_copy(
        send_a.at[pl.ds(me * 32, 32), :], recv_a.at[me], own_sem.at[0]
    )

    def own_b(zi):
        return pltpu.make_async_copy(
            send_b.at[pl.ds((me * PLANES + zi) * ROWS, ROWS), :],
            recv_b.at[zi * NB + me],
            own_sem.at[zi + 1],
        )

    def start_part(zi, sem, first, count):
        rows = pl.ds(first * 8, count * 8)

        def start(n):
            peer = band_peer(n)
            pltpu.make_async_remote_copy(
                src_ref=send_b.at[
                    pl.ds((peer * PLANES + zi) * ROWS + first * 8, count * 8), :
                ],
                dst_ref=recv_b.at[zi * NB + me, rows],
                send_sem=band_send.at[sem],
                recv_sem=band_recv.at[sem],
                device_id=(ka, peer),
                device_id_type=MESH,
            ).start()

        each(NB - 1, start)

    def wait_part(zi, sems, sem, first, count):
        wait_bytes(
            recv_b.at[pl.ds(zi * NB, NB - 1), pl.ds(first * 8, count * 8)], sems.at[sem]
        )

    def start_b(zi):
        start_part(zi, zi + 1, 0, REST)
        own_b(zi).start()

    def wait_b(zi, sems):
        wait_part(zi, sems, zi + 1, 0, REST)

    def start_slot(rows, slot, sem, device):
        pltpu.make_async_remote_copy(
            src_ref=rows.at[slot],
            dst_ref=rows.at[slot],
            send_sem=sem.at[0],
            recv_sem=sem.at[1],
            device_id=device,
            device_id_type=MESH,
        ).start()

    def wait_rows(rows, count, sem, side):
        wait_bytes(rows.at[pl.ds(0, count - 1)], sem.at[side])

    each(NB - 1, start_a)
    own_a.start()

    def store_b(b):
        def store(j, block):
            send_b[pl.ds((b - 1) * 8 + j, NG, stride=ROWS), :] = block

        return store

    other_psi.wait()
    each(REST, lambda i: transform(i + 1, store_b(i + 1)))
    loads[7].wait()
    own_weight = jnp.full((1, 128), weights[0].astype(jnp.float32))
    w_rows[ka] = own_weight
    start_b(0)

    loads[4].wait()

    def gram_step(h):
        product = resid[h].reshape(1, PLANES * NG // 8, 8, NG) * resid[...].reshape(
            HIST, PLANES * NG // 8, 8, NG
        )
        gram_part[pl.ds(pl.multiple_of(h * HIST, HIST), HIST), :] = jnp.sum(
            jnp.sum(product, axis=1), axis=1
        )

    each(HIST, gram_step)
    each(KA - 1, lambda n: start_slot(w_rows, ka, w_sem, (ka_peer(n), me)))
    gram_rows[me] = diagonal_row(gram_part[...])

    loads[5].wait()
    loads[6].wait()
    dens[...] = dens[...] + BETA * resid[...]
    proj_part[...] = jnp.zeros((HIST, 128), jnp.float32)

    start_b(1)
    each(NB - 1, lambda n: start_slot(gram_rows, me, gram_sem, (ka, band_peer(n))))

    wait_rows(w_rows, KA, w_sem, 1)
    factor = own_weight / jnp.sum(w_rows[...], axis=0) * jnp.float32(1.0 / NG**3)
    loads[2].wait()
    loads[3].wait()

    def operand_a(zi):
        return recv_a[:, pl.ds(pl.multiple_of(zi * 8, 8), 8), :].reshape(2 * NG, NG)

    def operand_b(zi, b):
        return recv_b[
            pl.ds(zi * NB, NB), pl.ds(pl.multiple_of((b - 1) * 8, 8), 8), :
        ].reshape(2 * NG, NG)

    def pair_power(left, right, b_left, b_right):
        field = times(xh[...], xl[...], jnp.concatenate([left, right], axis=1), 0)
        power = field[:NG] * field[:NG] + field[NG:] * field[NG:]
        return (
            power[:, :NG] * occ[0, b_left].astype(jnp.float32)
            + power[:, NG:] * occ[0, b_right].astype(jnp.float32)
        )

    def compute_plane(zi):
        plane_buf[zi] = pair_power(operand_a(zi), operand_b(zi, REST), 0, REST)

        def pair(i):
            b = 2 * i + 1
            plane_buf[zi] = plane_buf[zi] + pair_power(
                operand_b(zi, b), operand_b(zi, b + 1), b, b + 1
            )

        each(REST // 2, pair)
        plane_buf[zi] = plane_buf[zi] * factor

    def compute_last_plane(zi):
        wait_part(zi, band_recv, zi + 1, 0, REST - LATE)
        own_b(zi).wait()
        plane_buf[zi] = pair_power(operand_b(zi, 1), operand_b(zi, 2), 1, 2)

        def pair(i):
            b = 2 * i + 1
            plane_buf[zi] = plane_buf[zi] + pair_power(
                operand_b(zi, b), operand_b(zi, b + 1), b, b + 1
            )

        lax.fori_loop(1, (REST - LATE) // 2, lambda i, carry: (pair(i), carry)[1], 0)
        wait_part(zi, band_recv, zi + 2, REST - LATE, LATE)
        each(last, lambda early_zi: z_copy(early_zi).start())
        total = (
            plane_buf[zi]
            + pair_power(operand_b(zi, REST - 2), operand_b(zi, REST - 1), REST - 2, REST - 1)
            + pair_power(operand_a(zi), operand_b(zi, REST), 0, REST)
        )
        plane_buf[zi] = total * factor

    def start_rs(zi):
        def start(n):
            peer = x_peer(n)
            pltpu.make_async_remote_copy(
                src_ref=plane_buf.at[zi, pl.ds(peer * QUARTER, QUARTER), :],
                dst_ref=rs_buf.at[zi, x],
                send_sem=rs_send.at[zi],
                recv_sem=rs_recv.at[zi],
                device_id=(z_hi * XS + peer, me),
                device_id_type=MESH,
            ).start()

        each(XS - 1, start)

    def z_copy(zi):
        return pltpu.make_async_remote_copy(
            src_ref=z_send.at[zi],
            dst_ref=z_recv.at[zi],
            send_sem=z_ssem.at[zi],
            recv_sem=z_rsem.at[zi],
            device_id=(lax.rem(ka + XS, KA), me),
            device_id_type=MESH,
        )

    def add_up(zi):
        wait_bytes(rs_buf.at[zi, pl.ds(0, XS - 1)], rs_recv.at[zi])
        z_send[zi] = (
            plane_buf[zi, mine, :]
            + rs_buf[zi, lax.rem(x + 1, XS)]
            + rs_buf[zi, lax.rem(x + 2, XS)]
            + rs_buf[zi, lax.rem(x + 3, XS)]
        )

    def start_gather(zi):
        z_copy(zi).wait_recv()
        out_density[zi, mine, :] = z_send[zi] + z_recv[zi]

        def start(n):
            pltpu.make_async_remote_copy(
                src_ref=out_density.at[zi, mine, :],
                dst_ref=out_density.at[zi, mine, :],
                send_sem=ag_send.at[zi],
                recv_sem=ag_recv.at[zi],
                device_id=(z_hi * XS + x_peer(n), me),
                device_id_type=MESH,
            ).start()

        each(XS - 1, start)

    def project(zi):
        own = plane_buf[zi] - (1.0 / KA) * din[zi]
        product = (resid[:, zi] * own[None]).reshape(HIST, NG // 8, 8, NG)
        proj_part[...] = proj_part[...] + jnp.sum(jnp.sum(product, axis=1), axis=1)


    def invert():
        wait_rows(gram_rows, NB, gram_sem, 1)
        gram_part[...] = spread_rows(jnp.sum(gram_rows[...], axis=0), HIST * HIST)

        def entry(i, j):
            return gram_part[i * HIST + j : i * HIST + j + 1, :]

        lower, pivots = {}, []
        for j in range(HIST):
            pivot = entry(j, j) * (1.0 + REGULAR)
            for k in range(j):
                pivot = pivot - lower[j, k] * lower[j, k]
            pivots.append(1.0 / jnp.sqrt(pivot))
            for i in range(j + 1, HIST):
                value = entry(i, j)
                for k in range(j):
                    value = value - lower[i, k] * lower[j, k]
                lower[i, j] = value * pivots[j]
        unlower = {}
        for j in range(HIST):
            unlower[j, j] = pivots[j]
            for i in range(j + 1, HIST):
                value = lower[i, j] * unlower[j, j]
                for k in range(j + 1, i):
                    value = value + lower[i, k] * unlower[k, j]
                unlower[i, j] = -value * pivots[i]
        lane = lax.broadcasted_iota(jnp.int32, (1, 128), 1)
        for i in range(HIST):
            row = jnp.zeros((1, 128), jnp.float32)
            for j in range(HIST):
                value = sum(unlower[k, i] * unlower[k, j] for k in range(max(i, j), HIST))
                row = jnp.where(lane == j, value, row)
            inverse[i : i + 1, :] = row

    def early(zi):
        wait_b(zi, band_recv)
        own_b(zi).wait()
        compute_plane(zi)
        start_rs(zi)
        project(zi)
        add_up(zi)

        @pl.when(zi == 0)
        def _():
            start_b(2)

        @pl.when(zi == 1)
        def _():
            start_part(last, last + 1, 0, REST - LATE)
            own_b(last).start()
            start_part(last, last + 2, REST - LATE, LATE)

        @pl.when(zi == 1)
        def _():
            invert()

    wait_bytes(recv_a.at[pl.ds(0, NB - 1)], band_recv.at[0])
    own_a.wait()
    each(last, early)

    wait_bytes(recv_a.at[pl.ds(0, NB - 1)], band_send.at[0])
    for zi in range(PLANES - 2):
        wait_b(zi, band_send)
    wait_rows(w_rows, KA, w_sem, 0)
    wait_rows(gram_rows, NB, gram_sem, 0)

    compute_last_plane(last)
    start_rs(last)
    project(last)
    proj_rows[flat_slot] = diagonal_row(proj_part[...])
    for device in flat_peers:
        start_slot(proj_rows, flat_slot, proj_sem, device)
    add_up(last)
    z_copy(last).start()
    each(last, start_gather)
    wait_rows(proj_rows, NB, proj_sem, 1)
    total_rows[z_slot] = jnp.sum(proj_rows[...], axis=0)
    for device in z_peers:
        start_slot(total_rows, z_slot, total_sem, device)
    start_gather(last)

    wait_b(last - 1, band_send)
    wait_part(last, band_send, last + 1, 0, REST - LATE)
    wait_part(last, band_send, last + 2, REST - LATE, LATE)
    wait_rows(proj_rows, NB, proj_sem, 0)
    for zi in range(PLANES):
        wait_bytes(rs_buf.at[zi, pl.ds(0, XS - 1)], rs_send.at[zi])
        z_copy(zi).wait_send()

    wait_rows(total_rows, KA, total_sem, 1)
    projections = jnp.sum(total_rows[...], axis=0)
    coefs = jnp.sum(inverse[...] * projections, axis=1, keepdims=True)
    for zi in range(PLANES):
        wait_bytes(out_density.at[zi, pl.ds(0, NG - QUARTER), :], ag_recv.at[zi])
        update = coefs[0:1] * dens[0, zi]
        for h in range(1, HIST):
            update = update + coefs[h : h + 1] * dens[h, zi]
        out_mixed[zi] = din[zi] + BETA * (out_density[zi] - din[zi]) - update

    wait_rows(total_rows, KA, total_sem, 0)
    for zi in range(PLANES):
        wait_bytes(out_density.at[zi, pl.ds(0, NG - QUARTER), :], ag_send.at[zi])


def write_out(density, mixed, out_density, out_mixed, sems):
    copies = [
        pltpu.make_async_copy(density, out_density, sems.at[0]),
        pltpu.make_async_copy(mixed, out_mixed, sems.at[1]),
    ]
    for copy in copies:
        copy.start()
    for copy in copies:
        copy.wait()


def shards(psi_hat, occupations, weights, density_in, dens_hist, resid_hist):
    operands = (occupations, psi_hat, density_in, dens_hist, resid_hist)
    operands += tuple(jnp.asarray(table) for table in dft_tables())
    plane = (PLANES, NG, NG)
    f32 = jnp.float32
    dma = pltpu.SemaphoreType.DMA
    vmem = partial(pltpu.VMEM)
    hbm_spec = pl.BlockSpec(memory_space=pltpu.HBM)
    vmem_spec = pl.BlockSpec(memory_space=pltpu.VMEM)
    table = vmem((2 * NG, 2 * NG), jnp.bfloat16)
    density, mixed = pl.pallas_call(
        kernel,
        out_shape=(jax.ShapeDtypeStruct(plane, f32), jax.ShapeDtypeStruct(plane, f32)),
        in_specs=[pl.BlockSpec(memory_space=pltpu.SMEM)] + [hbm_spec] * 9,
        out_specs=(vmem_spec, vmem_spec),
        scratch_shapes=[
            pltpu.SMEM((1, BANDS), jnp.int32),
            vmem((BANDS, 2, PLANES, NG, NG), f32),
            vmem(plane, f32),
            vmem((HIST, *plane), f32),
            vmem((HIST, *plane), f32),
            table, table, table, table,
            vmem((NG * 8, NG), f32),
            vmem((NG * ROWS, NG), f32),
            vmem((NB, 8 * PLANES, NG), f32),
            vmem((PLANES * NB, ROWS, NG), f32),
            vmem(plane, f32),
            vmem((PLANES, XS, QUARTER, NG), f32),
            vmem((PLANES, QUARTER, NG), f32),
            vmem((PLANES, QUARTER, NG), f32),
            vmem((HIST * HIST, 128), f32),
            vmem((NB, 1, 128), f32),
            vmem((HIST, 128), f32),
            vmem((NB, 1, 128), f32),
            vmem((KA, 1, 128), f32),
            vmem((KA, 1, 128), f32),
            vmem((HIST, 128), f32),
            dma((2,)), dma((8,)), dma((CHUNKS,)),
            dma((CHUNKS,)), dma((CHUNKS,)),
            dma((PLANES,)), dma((PLANES,)),
            dma((PLANES,)), dma((PLANES,)),
            dma((PLANES,)), dma((PLANES,)),
            dma((2,)), dma((2,)), dma((2,)), dma((2,)),
        ],
        compiler_params=pltpu.CompilerParams(
            collective_id=0, has_side_effects=True, vmem_limit_bytes=32 * 1024 * 1024
        ),
    )(weights, *(pltpu.with_memory_space_constraint(operand, pltpu.HBM) for operand in operands))
    return pl.pallas_call(
        write_out,
        out_shape=(jax.ShapeDtypeStruct(plane, f32), jax.ShapeDtypeStruct(plane, f32)),
        in_specs=[vmem_spec, vmem_spec],
        out_specs=(hbm_spec, hbm_spec),
        scratch_shapes=[dma((2,))],
        compiler_params=pltpu.CompilerParams(vmem_limit_bytes=1024 * 1024),
    )(density, mixed)


def solution(mesh):
    return jax.shard_map(
        shards,
        mesh=mesh,
        in_specs=(
            P("ka", None, None, "band", None, None),
            P("ka", None),
            P("ka"),
            P("band", None, None),
            P(None, "band", None, None),
            P(None, "band", None, None),
        ),
        out_specs=(P("band", None, None), P("band", None, None)),
        check_vma=False,
    )
```

```python
from functools import partial

import jax
import jax.numpy as jnp
import ml_dtypes
import numpy as np
from jax import lax
from jax.experimental import pallas as pl
from jax.experimental.pallas import tpu as pltpu
from jax.sharding import PartitionSpec as P

NG = 128
BANDS = 12
HIST = 8
KA = 8
NB = 32
XS = 4
PLANES = NG // NB
REST = BANDS - 1
ROWS = REST * 8
QUARTER = NG // XS
LATE = 3
CHUNKS = PLANES + 2
BETA = 0.3
REGULAR = 0.01
MESH = pl.DeviceIdType.MESH


def split_table(table):
    high = table.astype(ml_dtypes.bfloat16)
    low = (table - high.astype(np.float64)).astype(ml_dtypes.bfloat16)
    return high, low


def dft_tables():
    index = np.arange(NG)
    angles = 2.0 * np.pi * (index[:, None] * index[None, :] % NG) / NG
    cosine, sine = np.cos(angles), np.sin(angles)
    table = np.block([[cosine, -sine], [sine, cosine]])
    order = [
        part * NG + source * PLANES + p
        for source in range(NB)
        for part in range(2)
        for p in range(PLANES)
    ]
    return (*split_table(table), *split_table(table[:, order]))


def split(x):
    high = x.astype(jnp.bfloat16)
    low = (x - high.astype(jnp.float32)).astype(jnp.bfloat16)
    return high, low


def times(table_high, table_low, x, contract):
    high, low = split(x)
    dot = partial(
        lax.dot_general,
        dimension_numbers=(((1,), (contract,)), ((), ())),
        preferred_element_type=jnp.float32,
    )
    return dot(table_high, high) + (dot(table_low, high) + dot(table_high, low))


def diagonal_row(columns):
    sums = jnp.sum(columns, axis=1, keepdims=True)
    shape = columns.shape
    on = lax.broadcasted_iota(jnp.int32, shape, 0) == lax.broadcasted_iota(jnp.int32, shape, 1)
    return jnp.sum(jnp.where(on, sums, 0.0), axis=0, keepdims=True)


def spread_rows(row, count):
    shape = (count, 128)
    on = lax.broadcasted_iota(jnp.int32, shape, 0) == lax.broadcasted_iota(jnp.int32, shape, 1)
    picked = jnp.sum(jnp.where(on, row, 0.0), axis=1, keepdims=True)
    return jnp.broadcast_to(picked, shape)


def kernel(
    weights, occ_hbm, psi, din_hbm, dens_hbm, resid_hbm, th_hbm, tl_hbm, xh_hbm, xl_hbm,
    out_density, out_mixed,
    occ, psi_v, din, dens, resid, th, tl, xh, xl,
    send_a, send_b, recv_a, recv_b,
    plane_buf, rs_buf, z_send, z_recv, gram_part, gram_rows, proj_part, proj_rows, total_rows, w_rows, inverse,
    psi_sem, load_sem, own_sem,
    band_send, band_recv, rs_send, rs_recv, z_ssem, z_rsem, ag_send, ag_recv,
    gram_sem, proj_sem, total_sem, w_sem,
):
    ka = lax.axis_index("ka")
    me = lax.axis_index("band")
    z_hi, x = lax.div(ka, XS), lax.rem(ka, XS)
    y, z, core = lax.div(me, 8), lax.rem(lax.div(me, 2), 4), lax.rem(me, 2)

    half = lax.div(z, 2)
    z_end, z_middle, z_beside = 3 - 3 * half, 2 - half, half * 2 + 1 - lax.rem(z, 2)

    def band_peer(n):
        i, dy = lax.div(n, 4), 3 - lax.rem(n, 4)
        z_far = jnp.where(lax.rem(i, 2) == 0, z_end, z_middle)
        z_near = jnp.where(i < 6, z_beside, z)
        core_near = jnp.where(i < 6, i - 4, jnp.where(i == 6, 1 - core, core))
        z_to = jnp.where(i < 4, z_far, z_near)
        core_to = jnp.where(i < 4, lax.div(i, 2), core_near)
        return lax.rem(y + dy, 4) * 8 + z_to * 2 + core_to

    y_part = [lax.rem(y + dy, 4) * 8 for dy in range(4)]
    core_part = [core, 1 - core]
    others_along_z = [z_end, z_middle, z_beside]

    def across(dx, dy, dc):
        return z_hi * XS + lax.rem(x + dx, XS), y_part[dy] + z * 2 + core_part[dc]

    flat = [(dx, dy, dc) for dx in range(XS) for dy in range(4) for dc in range(2)][1:]
    flat_peers = [across(*step) for step in flat]
    flat_slot = x * 8 + y * 2 + core
    z_slot = z_hi * 4 + z

    def along_z(dz):
        to = lax.rem(z_slot + dz, 8)
        return lax.div(to, 4) * XS + x, y * 8 + lax.rem(to, 4) * 2 + core

    z_peers = [along_z(dz) for dz in range(1, 8)]

    def ka_peer(n):
        return lax.rem(ka + 1 + n, KA)

    def each(count, body):
        def step(n, carry):
            body(n)
            return carry

        lax.fori_loop(0, count, step, 0)

    def wait_bytes(ref, sem):
        pltpu.make_async_copy(ref, ref, sem).wait()

    last = PLANES - 1
    mine = pl.ds(pl.multiple_of(x * QUARTER, QUARTER), QUARTER)

    first_psi = pltpu.make_async_copy(psi.at[0, 0], psi_v.at[0], psi_sem.at[0])
    other_psi = pltpu.make_async_copy(
        psi.at[0, pl.ds(1, REST)], psi_v.at[pl.ds(1, REST)], psi_sem.at[1]
    )
    loads = [
        pltpu.make_async_copy(src, dst, load_sem.at[i])
        for i, (src, dst) in enumerate(
            [
                (th_hbm, th), (tl_hbm, tl), (xh_hbm, xh), (xl_hbm, xl),
                (resid_hbm, resid), (dens_hbm, dens), (din_hbm, din),
                (occ_hbm, occ),
            ]
        )
    ]
    loads[0].start()
    first_psi.start()
    loads[1].start()

    barrier = pltpu.get_barrier_semaphore()
    for z_to in others_along_z:
        for dy, dc in [(dy, dc) for dy in range(4) for dc in range(2)][1:]:
            device = (ka, y_part[dy] + z_to * 2 + core_part[dc])
            pl.semaphore_signal(barrier, inc=1, device_id=device, device_id_type=MESH)
    other_half = XS - z_hi * XS
    for dx in range(1, XS):
        device = (other_half + lax.rem(x + dx, XS), me)
        pl.semaphore_signal(barrier, inc=1, device_id=device, device_id_type=MESH)
    for device in z_peers + flat_peers:
        pl.semaphore_signal(barrier, inc=1, device_id=device, device_id_type=MESH)

    other_psi.start()
    for load in loads[2:]:
        load.start()
    loads[0].wait()
    loads[1].wait()
    first_psi.wait()

    def transform(b, store):
        columns = jnp.concatenate(
            [
                jnp.concatenate([psi_v[b, 0, p], psi_v[b, 1, p]], axis=0)
                for p in range(PLANES)
            ],
            axis=1,
        )
        along_y = times(th[...], tl[...], columns, 0)
        rows = jnp.concatenate(
            [
                jnp.concatenate(
                    [
                        along_y[:NG, p * NG : (p + 1) * NG],
                        along_y[NG:, p * NG : (p + 1) * NG],
                    ],
                    axis=1,
                )
                for p in range(PLANES)
            ],
            axis=0,
        )
        along_z = times(th[...], tl[...], rows, 1)
        for part in range(2):
            for p in range(PLANES):
                store(
                    part * PLANES + p,
                    along_z[part * NG : (part + 1) * NG, p * NG : (p + 1) * NG],
                )

    def store_a(j, block):
        send_a[pl.ds(j, NG, stride=8), :] = block

    transform(0, store_a)
    pl.semaphore_wait(barrier, 7 + NB - 1 + XS - 1 + 21)

    def start_a(n):
        peer = band_peer(n)
        pltpu.make_async_remote_copy(
            src_ref=send_a.at[pl.ds(peer * 32, 32), :],
            dst_ref=recv_a.at[me],
            send_sem=band_send.at[0],
            recv_sem=band_recv.at[0],
            device_id=(ka, peer),
            device_id_type=MESH,
        ).start()

    own_a = pltpu.make_async_copy(
        send_a.at[pl.ds(me * 32, 32), :], recv_a.at[me], own_sem.at[0]
    )

    def own_b(zi):
        return pltpu.make_async_copy(
            send_b.at[pl.ds((me * PLANES + zi) * ROWS, ROWS), :],
            recv_b.at[zi * NB + me],
            own_sem.at[zi + 1],
        )

    def start_part(zi, sem, first, count):
        rows = pl.ds(first * 8, count * 8)

        def start(n):
            peer = band_peer(n)
            pltpu.make_async_remote_copy(
                src_ref=send_b.at[
                    pl.ds((peer * PLANES + zi) * ROWS + first * 8, count * 8), :
                ],
                dst_ref=recv_b.at[zi * NB + me, rows],
                send_sem=band_send.at[sem],
                recv_sem=band_recv.at[sem],
                device_id=(ka, peer),
                device_id_type=MESH,
            ).start()

        each(NB - 1, start)

    def wait_part(zi, sems, sem, first, count):
        wait_bytes(
            recv_b.at[pl.ds(zi * NB, NB - 1), pl.ds(first * 8, count * 8)], sems.at[sem]
        )

    def start_b(zi):
        start_part(zi, zi + 1, 0, REST)
        own_b(zi).start()

    def wait_b(zi, sems):
        wait_part(zi, sems, zi + 1, 0, REST)

    def start_slot(rows, slot, sem, device):
        pltpu.make_async_remote_copy(
            src_ref=rows.at[slot],
            dst_ref=rows.at[slot],
            send_sem=sem.at[0],
            recv_sem=sem.at[1],
            device_id=device,
            device_id_type=MESH,
        ).start()

    def wait_rows(rows, count, sem, side):
        wait_bytes(rows.at[pl.ds(0, count - 1)], sem.at[side])

    each(NB - 1, start_a)
    own_a.start()

    def store_b(b):
        def store(j, block):
            send_b[pl.ds((b - 1) * 8 + j, NG, stride=ROWS), :] = block

        return store

    other_psi.wait()
    each(REST, lambda i: transform(i + 1, store_b(i + 1)))
    loads[7].wait()
    own_weight = jnp.full((1, 128), weights[0].astype(jnp.float32))
    w_rows[ka] = own_weight
    start_b(0)

    loads[4].wait()

    def gram_step(h):
        product = resid[h].reshape(1, PLANES * NG // 8, 8, NG) * resid[...].reshape(
            HIST, PLANES * NG // 8, 8, NG
        )
        gram_part[pl.ds(pl.multiple_of(h * HIST, HIST), HIST), :] = jnp.sum(
            jnp.sum(product, axis=1), axis=1
        )

    each(HIST, gram_step)
    each(KA - 1, lambda n: start_slot(w_rows, ka, w_sem, (ka_peer(n), me)))
    gram_rows[me] = diagonal_row(gram_part[...])

    loads[5].wait()
    loads[6].wait()
    dens[...] = dens[...] + BETA * resid[...]
    proj_part[...] = jnp.zeros((HIST, 128), jnp.float32)

    start_b(1)
    each(NB - 1, lambda n: start_slot(gram_rows, me, gram_sem, (ka, band_peer(n))))

    wait_rows(w_rows, KA, w_sem, 1)
    factor = own_weight / jnp.sum(w_rows[...], axis=0) * jnp.float32(1.0 / NG**3)
    loads[2].wait()
    loads[3].wait()

    def operand_a(zi):
        return recv_a[:, pl.ds(pl.multiple_of(zi * 8, 8), 8), :].reshape(2 * NG, NG)

    def operand_b(zi, b):
        return recv_b[
            pl.ds(zi * NB, NB), pl.ds(pl.multiple_of((b - 1) * 8, 8), 8), :
        ].reshape(2 * NG, NG)

    def pair_power(left, right, b_left, b_right):
        field = times(xh[...], xl[...], jnp.concatenate([left, right], axis=1), 0)
        power = field[:NG] * field[:NG] + field[NG:] * field[NG:]
        return (
            power[:, :NG] * occ[0, b_left].astype(jnp.float32)
            + power[:, NG:] * occ[0, b_right].astype(jnp.float32)
        )

    def compute_plane(zi):
        plane_buf[zi] = pair_power(operand_a(zi), operand_b(zi, REST), 0, REST)

        def pair(i):
            b = 2 * i + 1
            plane_buf[zi] = plane_buf[zi] + pair_power(
                operand_b(zi, b), operand_b(zi, b + 1), b, b + 1
            )

        each(REST // 2, pair)
        plane_buf[zi] = plane_buf[zi] * factor

    def compute_last_plane(zi):
        wait_part(zi, band_recv, zi + 1, 0, REST - LATE)
        own_b(zi).wait()
        plane_buf[zi] = pair_power(operand_b(zi, 1), operand_b(zi, 2), 1, 2)

        def pair(i):
            b = 2 * i + 1
            plane_buf[zi] = plane_buf[zi] + pair_power(
                operand_b(zi, b), operand_b(zi, b + 1), b, b + 1
            )

        lax.fori_loop(1, (REST - LATE) // 2, lambda i, carry: (pair(i), carry)[1], 0)
        wait_part(zi, band_recv, zi + 2, REST - LATE, LATE)
        z_copy(0).start()
        total = (
            plane_buf[zi]
            + pair_power(operand_b(zi, REST - 2), operand_b(zi, REST - 1), REST - 2, REST - 1)
            + pair_power(operand_a(zi), operand_b(zi, REST), 0, REST)
        )
        plane_buf[zi] = total * factor

    def start_rs(zi):
        for dx in (2, 1, 3):
            device = across(dx, 0, 0)
            pltpu.make_async_remote_copy(
                src_ref=plane_buf.at[zi, pl.ds(lax.rem(x + dx, XS) * QUARTER, QUARTER), :],
                dst_ref=rs_buf.at[zi, x],
                send_sem=rs_send.at[zi],
                recv_sem=rs_recv.at[zi],
                device_id=device,
                device_id_type=MESH,
            ).start()

    groups = [pl.ds(0, last), pl.ds(last, 1)]

    def z_copy(group):
        return pltpu.make_async_remote_copy(
            src_ref=z_send.at[groups[group]],
            dst_ref=z_recv.at[groups[group]],
            send_sem=z_ssem.at[group],
            recv_sem=z_rsem.at[group],
            device_id=(lax.rem(ka + XS, KA), me),
            device_id_type=MESH,
        )

    def add_up(zi):
        wait_bytes(rs_buf.at[zi, pl.ds(0, XS - 1)], rs_recv.at[zi])
        z_send[zi] = (
            plane_buf[zi, mine, :]
            + rs_buf[zi, lax.rem(x + 1, XS)]
            + rs_buf[zi, lax.rem(x + 2, XS)]
            + rs_buf[zi, lax.rem(x + 3, XS)]
        )

    def start_gather(group):
        planes = groups[group]
        z_copy(group).wait_recv()
        out_density[planes, mine, :] = z_send[planes] + z_recv[planes]
        for dx in (2, 1, 3):
            pltpu.make_async_remote_copy(
                src_ref=out_density.at[planes, mine, :],
                dst_ref=out_density.at[planes, mine, :],
                send_sem=ag_send.at[group],
                recv_sem=ag_recv.at[group],
                device_id=across(dx, 0, 0),
                device_id_type=MESH,
            ).start()

    def wait_gather(group, sems):
        wait_bytes(out_density.at[groups[group], pl.ds(0, NG - QUARTER), :], sems.at[group])

    def project(zi):
        own = plane_buf[zi] - (1.0 / KA) * din[zi]
        product = (resid[:, zi] * own[None]).reshape(HIST, NG // 8, 8, NG)
        proj_part[...] = proj_part[...] + jnp.sum(jnp.sum(product, axis=1), axis=1)


    def invert():
        wait_rows(gram_rows, NB, gram_sem, 1)
        gram_part[...] = spread_rows(jnp.sum(gram_rows[...], axis=0), HIST * HIST)

        def entry(i, j):
            return gram_part[i * HIST + j : i * HIST + j + 1, :]

        lower, pivots = {}, []
        for j in range(HIST):
            pivot = entry(j, j) * (1.0 + REGULAR)
            for k in range(j):
                pivot = pivot - lower[j, k] * lower[j, k]
            pivots.append(1.0 / jnp.sqrt(pivot))
            for i in range(j + 1, HIST):
                value = entry(i, j)
                for k in range(j):
                    value = value - lower[i, k] * lower[j, k]
                lower[i, j] = value * pivots[j]
        unlower = {}
        for j in range(HIST):
            unlower[j, j] = pivots[j]
            for i in range(j + 1, HIST):
                value = lower[i, j] * unlower[j, j]
                for k in range(j + 1, i):
                    value = value + lower[i, k] * unlower[k, j]
                unlower[i, j] = -value * pivots[i]
        lane = lax.broadcasted_iota(jnp.int32, (1, 128), 1)
        for i in range(HIST):
            row = jnp.zeros((1, 128), jnp.float32)
            for j in range(HIST):
                value = sum(unlower[k, i] * unlower[k, j] for k in range(max(i, j), HIST))
                row = jnp.where(lane == j, value, row)
            inverse[i : i + 1, :] = row

    def early(zi):
        wait_b(zi, band_recv)
        own_b(zi).wait()
        compute_plane(zi)
        start_rs(zi)
        project(zi)
        add_up(zi)

        @pl.when(zi == 0)
        def _():
            start_b(2)

        @pl.when(zi == 1)
        def _():
            start_part(last, last + 1, 0, REST - LATE)
            own_b(last).start()
            start_part(last, last + 2, REST - LATE, LATE)

        @pl.when(zi == 1)
        def _():
            invert()

    wait_bytes(recv_a.at[pl.ds(0, NB - 1)], band_recv.at[0])
    own_a.wait()
    each(last, early)

    wait_bytes(recv_a.at[pl.ds(0, NB - 1)], band_send.at[0])
    for zi in range(PLANES - 2):
        wait_b(zi, band_send)
    wait_rows(w_rows, KA, w_sem, 0)
    wait_rows(gram_rows, NB, gram_sem, 0)

    compute_last_plane(last)
    start_rs(last)
    project(last)
    proj_rows[flat_slot] = diagonal_row(proj_part[...])
    for device in flat_peers:
        start_slot(proj_rows, flat_slot, proj_sem, device)
    add_up(last)
    z_copy(1).start()
    start_gather(0)
    wait_rows(proj_rows, NB, proj_sem, 1)
    total_rows[z_slot] = jnp.sum(proj_rows[...], axis=0)
    for device in z_peers:
        start_slot(total_rows, z_slot, total_sem, device)
    start_gather(1)

    wait_b(last - 1, band_send)
    wait_part(last, band_send, last + 1, 0, REST - LATE)
    wait_part(last, band_send, last + 2, REST - LATE, LATE)
    wait_rows(proj_rows, NB, proj_sem, 0)
    for zi in range(PLANES):
        wait_bytes(rs_buf.at[zi, pl.ds(0, XS - 1)], rs_send.at[zi])
    z_copy(0).wait_send()
    z_copy(1).wait_send()

    wait_rows(total_rows, KA, total_sem, 1)
    projections = jnp.sum(total_rows[...], axis=0)
    coefs = jnp.sum(inverse[...] * projections, axis=1, keepdims=True)
    for zi in range(PLANES):
        if zi == 0 or zi == last:
            wait_gather(zi // last, ag_recv)
        update = coefs[0:1] * dens[0, zi]
        for h in range(1, HIST):
            update = update + coefs[h : h + 1] * dens[h, zi]
        out_mixed[zi] = din[zi] + BETA * (out_density[zi] - din[zi]) - update

    wait_rows(total_rows, KA, total_sem, 0)
    wait_gather(0, ag_send)
    wait_gather(1, ag_send)


def write_out(density, mixed, out_density, out_mixed, sems):
    copies = [
        pltpu.make_async_copy(density, out_density, sems.at[0]),
        pltpu.make_async_copy(mixed, out_mixed, sems.at[1]),
    ]
    for copy in copies:
        copy.start()
    for copy in copies:
        copy.wait()


def shards(psi_hat, occupations, weights, density_in, dens_hist, resid_hist):
    operands = (occupations, psi_hat, density_in, dens_hist, resid_hist)
    operands += tuple(jnp.asarray(table) for table in dft_tables())
    plane = (PLANES, NG, NG)
    f32 = jnp.float32
    dma = pltpu.SemaphoreType.DMA
    vmem = partial(pltpu.VMEM)
    hbm_spec = pl.BlockSpec(memory_space=pltpu.HBM)
    vmem_spec = pl.BlockSpec(memory_space=pltpu.VMEM)
    table = vmem((2 * NG, 2 * NG), jnp.bfloat16)
    density, mixed = pl.pallas_call(
        kernel,
        out_shape=(jax.ShapeDtypeStruct(plane, f32), jax.ShapeDtypeStruct(plane, f32)),
        in_specs=[pl.BlockSpec(memory_space=pltpu.SMEM)] + [hbm_spec] * 9,
        out_specs=(vmem_spec, vmem_spec),
        scratch_shapes=[
            pltpu.SMEM((1, BANDS), jnp.int32),
            vmem((BANDS, 2, PLANES, NG, NG), f32),
            vmem(plane, f32),
            vmem((HIST, *plane), f32),
            vmem((HIST, *plane), f32),
            table, table, table, table,
            vmem((NG * 8, NG), f32),
            vmem((NG * ROWS, NG), f32),
            vmem((NB, 8 * PLANES, NG), f32),
            vmem((PLANES * NB, ROWS, NG), f32),
            vmem(plane, f32),
            vmem((PLANES, XS, QUARTER, NG), f32),
            vmem((PLANES, QUARTER, NG), f32),
            vmem((PLANES, QUARTER, NG), f32),
            vmem((HIST * HIST, 128), f32),
            vmem((NB, 1, 128), f32),
            vmem((HIST, 128), f32),
            vmem((NB, 1, 128), f32),
            vmem((KA, 1, 128), f32),
            vmem((KA, 1, 128), f32),
            vmem((HIST, 128), f32),
            dma((2,)), dma((8,)), dma((CHUNKS,)),
            dma((CHUNKS,)), dma((CHUNKS,)),
            dma((PLANES,)), dma((PLANES,)),
            dma((2,)), dma((2,)), dma((2,)), dma((2,)),
            dma((2,)), dma((2,)), dma((2,)), dma((2,)),
        ],
        compiler_params=pltpu.CompilerParams(
            collective_id=0, has_side_effects=True, vmem_limit_bytes=32 * 1024 * 1024
        ),
    )(weights, *(pltpu.with_memory_space_constraint(operand, pltpu.HBM) for operand in operands))
    return pl.pallas_call(
        write_out,
        out_shape=(jax.ShapeDtypeStruct(plane, f32), jax.ShapeDtypeStruct(plane, f32)),
        in_specs=[vmem_spec, vmem_spec],
        out_specs=(hbm_spec, hbm_spec),
        scratch_shapes=[dma((2,))],
        compiler_params=pltpu.CompilerParams(vmem_limit_bytes=1024 * 1024),
    )(density, mixed)


def solution(mesh):
    return jax.shard_map(
        shards,
        mesh=mesh,
        in_specs=(
            P("ka", None, None, "band", None, None),
            P("ka", None),
            P("ka"),
            P("band", None, None),
            P(None, "band", None, None),
            P(None, "band", None, None),
        ),
        out_specs=(P("band", None, None), P("band", None, None)),
        check_vma=False,
    )
```

```python
from functools import partial

import jax
import jax.numpy as jnp
import ml_dtypes
import numpy as np
from jax import lax
from jax.experimental import pallas as pl
from jax.experimental.pallas import tpu as pltpu
from jax.sharding import PartitionSpec as P

NG = 128
BANDS = 12
HIST = 8
KA = 8
NB = 32
XS = 4
PLANES = NG // NB
REST = BANDS - 1
ROWS = REST * 8
QUARTER = NG // XS
LATE = 3
CHUNKS = PLANES + 2
BETA = 0.3
REGULAR = 0.01
MESH = pl.DeviceIdType.MESH


def split_table(table):
    high = table.astype(ml_dtypes.bfloat16)
    low = (table - high.astype(np.float64)).astype(ml_dtypes.bfloat16)
    return high, low


def dft_tables():
    index = np.arange(NG)
    angles = 2.0 * np.pi * (index[:, None] * index[None, :] % NG) / NG
    cosine, sine = np.cos(angles), np.sin(angles)
    table = np.block([[cosine, -sine], [sine, cosine]])
    order = [
        part * NG + source * PLANES + p
        for source in range(NB)
        for part in range(2)
        for p in range(PLANES)
    ]
    return (*split_table(table), *split_table(table[:, order]))


def split(x):
    high = x.astype(jnp.bfloat16)
    low = (x - high.astype(jnp.float32)).astype(jnp.bfloat16)
    return high, low


def times(table_high, table_low, x, contract):
    high, low = split(x)
    dot = partial(
        lax.dot_general,
        dimension_numbers=(((1,), (contract,)), ((), ())),
        preferred_element_type=jnp.float32,
    )
    return dot(table_high, high) + (dot(table_low, high) + dot(table_high, low))


def diagonal_row(columns):
    sums = jnp.sum(columns, axis=1, keepdims=True)
    shape = columns.shape
    on = lax.broadcasted_iota(jnp.int32, shape, 0) == lax.broadcasted_iota(jnp.int32, shape, 1)
    return jnp.sum(jnp.where(on, sums, 0.0), axis=0, keepdims=True)


def spread_rows(row, count):
    shape = (count, 128)
    on = lax.broadcasted_iota(jnp.int32, shape, 0) == lax.broadcasted_iota(jnp.int32, shape, 1)
    picked = jnp.sum(jnp.where(on, row, 0.0), axis=1, keepdims=True)
    return jnp.broadcast_to(picked, shape)


def kernel(
    weights, occ_hbm, psi, din_hbm, dens_hbm, resid_hbm, th_hbm, tl_hbm, xh_hbm, xl_hbm,
    out_density, out_mixed,
    occ, psi_v, din, dens, resid, th, tl, xh, xl,
    send_a, send_b, recv_a, recv_b,
    plane_buf, rs_buf, z_send, z_recv, gram_part, gram_rows, proj_part, proj_rows, total_rows, w_rows, inverse,
    psi_sem, load_sem, own_sem,
    band_send, band_recv, rs_send, rs_recv, z_ssem, z_rsem, ag_send, ag_recv,
    gram_sem, proj_sem, total_sem, w_sem,
):
    ka = lax.axis_index("ka")
    me = lax.axis_index("band")
    z_hi, x = lax.div(ka, XS), lax.rem(ka, XS)
    y, z, core = lax.div(me, 8), lax.rem(lax.div(me, 2), 4), lax.rem(me, 2)

    half = lax.div(z, 2)
    z_end, z_middle, z_beside = 3 - 3 * half, 2 - half, half * 2 + 1 - lax.rem(z, 2)

    def band_peer(n):
        i, dy = lax.div(n, 4), 3 - lax.rem(n, 4)
        z_far = jnp.where(lax.rem(i, 2) == 0, z_end, z_middle)
        z_near = jnp.where(i < 6, z_beside, z)
        core_near = jnp.where(i < 6, i - 4, jnp.where(i == 6, 1 - core, core))
        z_to = jnp.where(i < 4, z_far, z_near)
        core_to = jnp.where(i < 4, lax.div(i, 2), core_near)
        return lax.rem(y + dy, 4) * 8 + z_to * 2 + core_to

    y_part = [lax.rem(y + dy, 4) * 8 for dy in range(4)]
    core_part = [core, 1 - core]
    others_along_z = [z_end, z_middle, z_beside]

    def across(dx, dy, dc):
        return z_hi * XS + lax.rem(x + dx, XS), y_part[dy] + z * 2 + core_part[dc]

    flat = [(dx, dy, dc) for dx in range(XS) for dy in range(4) for dc in range(2)][1:]
    flat_peers = [across(*step) for step in flat]
    flat_slot = x * 8 + y * 2 + core
    z_slot = z_hi * 4 + z

    def along_z(dz):
        to = lax.rem(z_slot + dz, 8)
        return lax.div(to, 4) * XS + x, y * 8 + lax.rem(to, 4) * 2 + core

    z_peers = [along_z(dz) for dz in range(1, 8)]

    def ka_peer(n):
        return lax.rem(ka + 1 + n, KA)

    def each(count, body):
        def step(n, carry):
            body(n)
            return carry

        lax.fori_loop(0, count, step, 0)

    def wait_bytes(ref, sem):
        pltpu.make_async_copy(ref, ref, sem).wait()

    last = PLANES - 1
    mine = pl.ds(pl.multiple_of(x * QUARTER, QUARTER), QUARTER)

    first_psi = pltpu.make_async_copy(psi.at[0, 0], psi_v.at[0], psi_sem.at[0])
    other_psi = pltpu.make_async_copy(
        psi.at[0, pl.ds(1, REST)], psi_v.at[pl.ds(1, REST)], psi_sem.at[1]
    )
    loads = [
        pltpu.make_async_copy(src, dst, load_sem.at[i])
        for i, (src, dst) in enumerate(
            [
                (th_hbm, th), (tl_hbm, tl), (xh_hbm, xh), (xl_hbm, xl),
                (resid_hbm, resid), (dens_hbm, dens), (din_hbm, din),
                (occ_hbm, occ),
            ]
        )
    ]
    loads[0].start()
    first_psi.start()
    loads[1].start()

    barrier = pltpu.get_barrier_semaphore()
    for z_to in others_along_z:
        for dy, dc in [(dy, dc) for dy in range(4) for dc in range(2)][1:]:
            device = (ka, y_part[dy] + z_to * 2 + core_part[dc])
            pl.semaphore_signal(barrier, inc=1, device_id=device, device_id_type=MESH)
    other_half = XS - z_hi * XS
    for dx in range(1, XS):
        device = (other_half + lax.rem(x + dx, XS), me)
        pl.semaphore_signal(barrier, inc=1, device_id=device, device_id_type=MESH)
    for device in z_peers + flat_peers:
        pl.semaphore_signal(barrier, inc=1, device_id=device, device_id_type=MESH)

    other_psi.start()
    for load in loads[2:]:
        load.start()
    loads[0].wait()
    loads[1].wait()
    first_psi.wait()

    def transform(b, store):
        columns = jnp.concatenate(
            [
                jnp.concatenate([psi_v[b, 0, p], psi_v[b, 1, p]], axis=0)
                for p in range(PLANES)
            ],
            axis=1,
        )
        along_y = times(th[...], tl[...], columns, 0)
        rows = jnp.concatenate(
            [
                jnp.concatenate(
                    [
                        along_y[:NG, p * NG : (p + 1) * NG],
                        along_y[NG:, p * NG : (p + 1) * NG],
                    ],
                    axis=1,
                )
                for p in range(PLANES)
            ],
            axis=0,
        )
        along_z = times(th[...], tl[...], rows, 1)
        for part in range(2):
            for p in range(PLANES):
                store(
                    part * PLANES + p,
                    along_z[part * NG : (part + 1) * NG, p * NG : (p + 1) * NG],
                )

    def store_a(j, block):
        send_a[pl.ds(j, NG, stride=8), :] = block

    transform(0, store_a)
    pl.semaphore_wait(barrier, 7 + NB - 1 + XS - 1 + 21)

    def start_a(n):
        peer = band_peer(n)
        pltpu.make_async_remote_copy(
            src_ref=send_a.at[pl.ds(peer * 32, 32), :],
            dst_ref=recv_a.at[me],
            send_sem=band_send.at[0],
            recv_sem=band_recv.at[0],
            device_id=(ka, peer),
            device_id_type=MESH,
        ).start()

    own_a = pltpu.make_async_copy(
        send_a.at[pl.ds(me * 32, 32), :], recv_a.at[me], own_sem.at[0]
    )

    def own_b(zi):
        return pltpu.make_async_copy(
            send_b.at[pl.ds((me * PLANES + zi) * ROWS, ROWS), :],
            recv_b.at[zi * NB + me],
            own_sem.at[zi + 1],
        )

    def start_part(zi, sem, first, count):
        rows = pl.ds(first * 8, count * 8)

        def start(n):
            peer = band_peer(n)
            pltpu.make_async_remote_copy(
                src_ref=send_b.at[
                    pl.ds((peer * PLANES + zi) * ROWS + first * 8, count * 8), :
                ],
                dst_ref=recv_b.at[zi * NB + me, rows],
                send_sem=band_send.at[sem],
                recv_sem=band_recv.at[sem],
                device_id=(ka, peer),
                device_id_type=MESH,
            ).start()

        each(NB - 1, start)

    def wait_part(zi, sems, sem, first, count):
        wait_bytes(
            recv_b.at[pl.ds(zi * NB, NB - 1), pl.ds(first * 8, count * 8)], sems.at[sem]
        )

    def start_b(zi):
        start_part(zi, zi + 1, 0, REST)
        own_b(zi).start()

    def wait_b(zi, sems):
        wait_part(zi, sems, zi + 1, 0, REST)

    def start_slot(rows, slot, sem, device):
        pltpu.make_async_remote_copy(
            src_ref=rows.at[slot],
            dst_ref=rows.at[slot],
            send_sem=sem.at[0],
            recv_sem=sem.at[1],
            device_id=device,
            device_id_type=MESH,
        ).start()

    def wait_rows(rows, count, sem, side):
        wait_bytes(rows.at[pl.ds(0, count - 1)], sem.at[side])

    each(NB - 1, start_a)
    own_a.start()

    def store_b(b):
        def store(j, block):
            send_b[pl.ds((b - 1) * 8 + j, NG, stride=ROWS), :] = block

        return store

    other_psi.wait()
    each(REST, lambda i: transform(i + 1, store_b(i + 1)))
    loads[7].wait()
    own_weight = jnp.full((1, 128), weights[0].astype(jnp.float32))
    w_rows[ka] = own_weight
    start_b(0)

    loads[4].wait()

    def gram_step(h):
        product = resid[h].reshape(1, PLANES * NG // 8, 8, NG) * resid[...].reshape(
            HIST, PLANES * NG // 8, 8, NG
        )
        gram_part[pl.ds(pl.multiple_of(h * HIST, HIST), HIST), :] = jnp.sum(
            jnp.sum(product, axis=1), axis=1
        )

    each(HIST, gram_step)
    each(KA - 1, lambda n: start_slot(w_rows, ka, w_sem, (ka_peer(n), me)))
    gram_rows[me] = diagonal_row(gram_part[...])

    loads[5].wait()
    loads[6].wait()
    dens[...] = dens[...] + BETA * resid[...]
    proj_part[...] = jnp.zeros((HIST, 128), jnp.float32)

    start_b(1)
    each(NB - 1, lambda n: start_slot(gram_rows, me, gram_sem, (ka, band_peer(n))))

    wait_rows(w_rows, KA, w_sem, 1)
    factor = own_weight / jnp.sum(w_rows[...], axis=0) * jnp.float32(1.0 / NG**3)
    loads[2].wait()
    loads[3].wait()

    def operand_a(zi):
        return recv_a[:, pl.ds(pl.multiple_of(zi * 8, 8), 8), :].reshape(2 * NG, NG)

    def operand_b(zi, b):
        return recv_b[
            pl.ds(zi * NB, NB), pl.ds(pl.multiple_of((b - 1) * 8, 8), 8), :
        ].reshape(2 * NG, NG)

    def pair_power(left, right, b_left, b_right):
        field = times(xh[...], xl[...], jnp.concatenate([left, right], axis=1), 0)
        power = field[:NG] * field[:NG] + field[NG:] * field[NG:]
        return (
            power[:, :NG] * occ[0, b_left].astype(jnp.float32)
            + power[:, NG:] * occ[0, b_right].astype(jnp.float32)
        )

    def compute_plane(zi):
        plane_buf[zi] = pair_power(operand_a(zi), operand_b(zi, REST), 0, REST)

        def pair(i):
            b = 2 * i + 1
            plane_buf[zi] = plane_buf[zi] + pair_power(
                operand_b(zi, b), operand_b(zi, b + 1), b, b + 1
            )

        each(REST // 2, pair)
        plane_buf[zi] = plane_buf[zi] * factor

    def compute_last_plane(zi):
        wait_part(zi, band_recv, zi + 1, 0, REST - LATE)
        own_b(zi).wait()
        plane_buf[zi] = pair_power(operand_b(zi, 1), operand_b(zi, 2), 1, 2)

        def pair(i):
            b = 2 * i + 1
            plane_buf[zi] = plane_buf[zi] + pair_power(
                operand_b(zi, b), operand_b(zi, b + 1), b, b + 1
            )

        lax.fori_loop(1, (REST - LATE) // 2, lambda i, carry: (pair(i), carry)[1], 0)
        wait_part(zi, band_recv, zi + 2, REST - LATE, LATE)
        z_copy(0).start()
        total = (
            plane_buf[zi]
            + pair_power(operand_b(zi, REST - 2), operand_b(zi, REST - 1), REST - 2, REST - 1)
            + pair_power(operand_a(zi), operand_b(zi, REST), 0, REST)
        )
        plane_buf[zi] = total * factor

    def start_rs(zi):
        for dx in (2, 1, 3):
            device = across(dx, 0, 0)
            pltpu.make_async_remote_copy(
                src_ref=plane_buf.at[zi, pl.ds(lax.rem(x + dx, XS) * QUARTER, QUARTER), :],
                dst_ref=rs_buf.at[zi, x],
                send_sem=rs_send.at[zi],
                recv_sem=rs_recv.at[zi],
                device_id=device,
                device_id_type=MESH,
            ).start()

    groups = [pl.ds(0, last), pl.ds(last, 1)]

    def z_copy(group):
        return pltpu.make_async_remote_copy(
            src_ref=z_send.at[groups[group]],
            dst_ref=z_recv.at[groups[group]],
            send_sem=z_ssem.at[group],
            recv_sem=z_rsem.at[group],
            device_id=(lax.rem(ka + XS, KA), me),
            device_id_type=MESH,
        )

    def add_up(zi):
        wait_bytes(rs_buf.at[zi, pl.ds(0, XS - 1)], rs_recv.at[zi])
        z_send[zi] = (
            plane_buf[zi, mine, :]
            + rs_buf[zi, lax.rem(x + 1, XS)]
            + rs_buf[zi, lax.rem(x + 2, XS)]
            + rs_buf[zi, lax.rem(x + 3, XS)]
        )

    def start_gather(group):
        planes = groups[group]
        z_copy(group).wait_recv()
        out_density[planes, mine, :] = z_send[planes] + z_recv[planes]
        for dx in (2, 1, 3):
            pltpu.make_async_remote_copy(
                src_ref=out_density.at[planes, mine, :],
                dst_ref=out_density.at[planes, mine, :],
                send_sem=ag_send.at[group],
                recv_sem=ag_recv.at[group],
                device_id=across(dx, 0, 0),
                device_id_type=MESH,
            ).start()

    def wait_gather(group, sems):
        wait_bytes(out_density.at[groups[group], pl.ds(0, NG - QUARTER), :], sems.at[group])

    def project(zi):
        own = plane_buf[zi] - (1.0 / KA) * din[zi]
        product = (resid[:, zi] * own[None]).reshape(HIST, NG // 8, 8, NG)
        proj_part[...] = proj_part[...] + jnp.sum(jnp.sum(product, axis=1), axis=1)


    def invert():
        wait_rows(gram_rows, NB, gram_sem, 1)
        gram_part[...] = spread_rows(jnp.sum(gram_rows[...], axis=0), HIST * HIST)

        def entry(i, j):
            return gram_part[i * HIST + j : i * HIST + j + 1, :]

        lower, pivots = {}, []
        for j in range(HIST):
            pivot = entry(j, j) * (1.0 + REGULAR)
            for k in range(j):
                pivot = pivot - lower[j, k] * lower[j, k]
            pivots.append(1.0 / jnp.sqrt(pivot))
            for i in range(j + 1, HIST):
                value = entry(i, j)
                for k in range(j):
                    value = value - lower[i, k] * lower[j, k]
                lower[i, j] = value * pivots[j]
        unlower = {}
        for j in range(HIST):
            unlower[j, j] = pivots[j]
            for i in range(j + 1, HIST):
                value = lower[i, j] * unlower[j, j]
                for k in range(j + 1, i):
                    value = value + lower[i, k] * unlower[k, j]
                unlower[i, j] = -value * pivots[i]
        lane = lax.broadcasted_iota(jnp.int32, (1, 128), 1)
        for i in range(HIST):
            row = jnp.zeros((1, 128), jnp.float32)
            for j in range(HIST):
                value = sum(unlower[k, i] * unlower[k, j] for k in range(max(i, j), HIST))
                row = jnp.where(lane == j, value, row)
            inverse[i : i + 1, :] = row

    def early(zi):
        wait_b(zi, band_recv)
        own_b(zi).wait()
        compute_plane(zi)
        start_rs(zi)
        project(zi)
        add_up(zi)

        @pl.when(zi == 0)
        def _():
            start_b(2)

        @pl.when(zi == 1)
        def _():
            start_part(last, last + 1, 0, REST - LATE)
            own_b(last).start()
            start_part(last, last + 2, REST - LATE, LATE)

        @pl.when(zi == 1)
        def _():
            invert()

    wait_bytes(recv_a.at[pl.ds(0, NB - 1)], band_recv.at[0])
    own_a.wait()
    each(last, early)

    wait_bytes(recv_a.at[pl.ds(0, NB - 1)], band_send.at[0])
    for zi in range(PLANES - 2):
        wait_b(zi, band_send)
    wait_rows(w_rows, KA, w_sem, 0)
    wait_rows(gram_rows, NB, gram_sem, 0)

    compute_last_plane(last)
    start_rs(last)
    project(last)
    proj_rows[flat_slot] = diagonal_row(proj_part[...])
    for device in flat_peers:
        start_slot(proj_rows, flat_slot, proj_sem, device)
    add_up(last)
    z_copy(1).start()
    wait_rows(proj_rows, NB, proj_sem, 1)
    total_rows[z_slot] = jnp.sum(proj_rows[...], axis=0)
    for device in z_peers:
        start_slot(total_rows, z_slot, total_sem, device)
    start_gather(0)
    start_gather(1)

    wait_b(last - 1, band_send)
    wait_part(last, band_send, last + 1, 0, REST - LATE)
    wait_part(last, band_send, last + 2, REST - LATE, LATE)
    wait_rows(proj_rows, NB, proj_sem, 0)
    for zi in range(PLANES):
        wait_bytes(rs_buf.at[zi, pl.ds(0, XS - 1)], rs_send.at[zi])
    z_copy(0).wait_send()
    z_copy(1).wait_send()

    wait_rows(total_rows, KA, total_sem, 1)
    projections = jnp.sum(total_rows[...], axis=0)
    coefs = jnp.sum(inverse[...] * projections, axis=1, keepdims=True)
    for zi in range(PLANES):
        if zi == 0 or zi == last:
            wait_gather(zi // last, ag_recv)
        update = coefs[0:1] * dens[0, zi]
        for h in range(1, HIST):
            update = update + coefs[h : h + 1] * dens[h, zi]
        out_mixed[zi] = din[zi] + BETA * (out_density[zi] - din[zi]) - update

    wait_rows(total_rows, KA, total_sem, 0)
    wait_gather(0, ag_send)
    wait_gather(1, ag_send)


def write_out(density, mixed, out_density, out_mixed, sems):
    copies = [
        pltpu.make_async_copy(density, out_density, sems.at[0]),
        pltpu.make_async_copy(mixed, out_mixed, sems.at[1]),
    ]
    for copy in copies:
        copy.start()
    for copy in copies:
        copy.wait()


def shards(psi_hat, occupations, weights, density_in, dens_hist, resid_hist):
    operands = (occupations, psi_hat, density_in, dens_hist, resid_hist)
    operands += tuple(jnp.asarray(table) for table in dft_tables())
    plane = (PLANES, NG, NG)
    f32 = jnp.float32
    dma = pltpu.SemaphoreType.DMA
    vmem = partial(pltpu.VMEM)
    hbm_spec = pl.BlockSpec(memory_space=pltpu.HBM)
    vmem_spec = pl.BlockSpec(memory_space=pltpu.VMEM)
    table = vmem((2 * NG, 2 * NG), jnp.bfloat16)
    density, mixed = pl.pallas_call(
        kernel,
        out_shape=(jax.ShapeDtypeStruct(plane, f32), jax.ShapeDtypeStruct(plane, f32)),
        in_specs=[pl.BlockSpec(memory_space=pltpu.SMEM)] + [hbm_spec] * 9,
        out_specs=(vmem_spec, vmem_spec),
        scratch_shapes=[
            pltpu.SMEM((1, BANDS), jnp.int32),
            vmem((BANDS, 2, PLANES, NG, NG), f32),
            vmem(plane, f32),
            vmem((HIST, *plane), f32),
            vmem((HIST, *plane), f32),
            table, table, table, table,
            vmem((NG * 8, NG), f32),
            vmem((NG * ROWS, NG), f32),
            vmem((NB, 8 * PLANES, NG), f32),
            vmem((PLANES * NB, ROWS, NG), f32),
            vmem(plane, f32),
            vmem((PLANES, XS, QUARTER, NG), f32),
            vmem((PLANES, QUARTER, NG), f32),
            vmem((PLANES, QUARTER, NG), f32),
            vmem((HIST * HIST, 128), f32),
            vmem((NB, 1, 128), f32),
            vmem((HIST, 128), f32),
            vmem((NB, 1, 128), f32),
            vmem((KA, 1, 128), f32),
            vmem((KA, 1, 128), f32),
            vmem((HIST, 128), f32),
            dma((2,)), dma((8,)), dma((CHUNKS,)),
            dma((CHUNKS,)), dma((CHUNKS,)),
            dma((PLANES,)), dma((PLANES,)),
            dma((2,)), dma((2,)), dma((2,)), dma((2,)),
            dma((2,)), dma((2,)), dma((2,)), dma((2,)),
        ],
        compiler_params=pltpu.CompilerParams(
            collective_id=0, has_side_effects=True, vmem_limit_bytes=32 * 1024 * 1024
        ),
    )(weights, *(pltpu.with_memory_space_constraint(operand, pltpu.HBM) for operand in operands))
    return pl.pallas_call(
        write_out,
        out_shape=(jax.ShapeDtypeStruct(plane, f32), jax.ShapeDtypeStruct(plane, f32)),
        in_specs=[vmem_spec, vmem_spec],
        out_specs=(hbm_spec, hbm_spec),
        scratch_shapes=[dma((2,))],
        compiler_params=pltpu.CompilerParams(vmem_limit_bytes=1024 * 1024),
    )(density, mixed)


def solution(mesh):
    return jax.shard_map(
        shards,
        mesh=mesh,
        in_specs=(
            P("ka", None, None, "band", None, None),
            P("ka", None),
            P("ka"),
            P("band", None, None),
            P(None, "band", None, None),
            P(None, "band", None, None),
        ),
        out_specs=(P("band", None, None), P("band", None, None)),
        check_vma=False,
    )
```
